128 devices in a mesh: gx: 4 (over y_hi, core), gy: 4 (over x), gz: 8 (over y_lo, z).
Axes of the slice: x: 4, y: 4 (y_hi: 2, y_lo: 2; y = y_hi * 2 + y_lo), z: 4, core: 2. Of those that a mesh axis runs over, the one named last changes fastest.
Arguments:
- features: float32 [64, 64, 256, 128], P('gx', 'gy', 'gz'), may hold values from -6 to 6
- scales: float32 [64, 64, 256], P('gx', 'gy', 'gz'), may hold values from 0.2 to 0.4
- thetas: float32 [2, 4, 128], replicated, may hold values from -1 to 1
- weights: float32 [2, 128, 128], replicated, may hold values from -0.5 to 0.5
Outputs:
- hidden: float32 [64, 64, 256, 128], P('gx', 'gy', 'gz')
The draws below stay inside these ranges and needn't reach their ends.
All inputs are finite; a program needn't handle non-finite values.
Results may differ from the reference program's by a relative error of at most 0.00011.
Values sent between devices are 32-bit elements; how exact they have to be, the bound alone decides.
No kernel may reach another device: no remote copies, remote signals or barrier semaphores. Data moves between devices by JAX's collectives and lax.ppermute only.
A program may use at most 64 MiB of HBM per device.

```python
import jax
import jax.numpy as jnp
from jax import lax

C = 128
ORDER = 3
LAYERS = 2
NX = 64
NY = 64
NZ = 256


def levels(key, extent, split, low, top_value):
    def one(dim, shards_of):
        draws = jax.random.uniform(jax.random.fold_in(jax.random.fold_in(key, 6), dim), (shards_of,), jnp.float32, low / len(split), top_value / len(split))
        return jnp.repeat(jnp.exp(draws), extent[dim] // shards_of).reshape((-1,) + (1,) * (len(extent) - dim - 1))

    gain = one(*split[0])
    for cut in split[1:]:
        gain = gain * one(*cut)
    return gain


def gaussian(rng, shape, deviation, most, pieces=(), kind=jnp.bfloat16):
    level = levels(rng, shape, pieces, -0.22, 0.18) if pieces else 1.0
    drawn = jax.random.normal(rng, shape, jnp.float32) * deviation * level
    return jnp.minimum(jnp.maximum(drawn, -most), most).astype(kind)


def setup_inputs(seed: int = 0) -> dict:
    key_of = jax.random.split(jax.random.key(seed), 5)
    return {
        "features": gaussian(key_of[0], (NX, NY, NZ, C), 1.0, 6.0, ((0, 4), (1, 4), (2, 8)), jnp.float32),
        "scales": jnp.clip(0.2 + 0.2 * jax.random.uniform(key_of[1], (NX, NY, NZ), jnp.float32) ** levels(key_of[1], (NX, NY, NZ), ((0, 4), (1, 4), (2, 8)), -0.2, 0.2), 0.2, 0.4),
        "thetas": jnp.clip(jax.random.uniform(key_of[2], (LAYERS, ORDER + 1, C), jnp.float32, -1.0, 1.0), -1.0, 1.0),
        "weights": gaussian(key_of[3], (LAYERS, C, C), C ** -0.5, 0.5, (), jnp.float32),
    }


def neighbour_sum(scaled):
    total = jnp.roll(scaled, 1, 0) + jnp.roll(scaled, -1, 0)
    total = total + jnp.roll(scaled, 1, 1) + jnp.roll(scaled, -1, 1)
    total = total + jnp.roll(scaled, 1, 2) + jnp.roll(scaled, -1, 2)
    return total


def operate(values_in, scales):
    scaled = scales[..., None] * values_in
    return -scales[..., None] * neighbour_sum(scaled)


def reference(features, scales, thetas, weights):
    hidden = features
    for layer_index in range(LAYERS):
        prior_term = hidden
        this_term = operate(hidden, scales)
        total = thetas[layer_index, 0] * prior_term + thetas[layer_index, 1] * this_term
        for order_index in range(2, ORDER + 1):
            next_term = 2.0 * operate(this_term, scales) - prior_term
            total = total + thetas[layer_index, order_index] * next_term
            prior_term, this_term = this_term, next_term
        flat = total.reshape(-1, total.shape[-1])
        mixed = jnp.dot(flat, weights[layer_index], precision=lax.Precision.HIGHEST, preferred_element_type=jnp.float32)
        hidden = jax.nn.silu(mixed).reshape(total.shape)
    return hidden
```

```python
import functools

import jax
import jax.numpy as jnp
from jax import lax
from jax.experimental import pallas as pl
from jax.experimental.pallas import tpu as pltpu
from jax.sharding import PartitionSpec as P


AXES = ("gx", "gy", "gz")
NX, NY, NZ, C = 16, 16, 32, 128
PLANE = NY * NZ
ROWS = NX * PLANE
FACE = {"gx": PLANE, "gy": NX * NZ, "gz": NX * NY}
SWAPS = (("gx", 1), ("gy", 0), ("gy", 1), ("gz", 0), ("gz", 1), ("gx", 0))

F32 = jnp.float32
VM = pl.BlockSpec(memory_space=pltpu.VMEM)
HBM = pl.BlockSpec(memory_space=pltpu.HBM)
MIB = 1024 * 1024


def arr(rows, cols=C, dtype=F32):
    return jax.ShapeDtypeStruct((rows, cols), dtype)


FACES_OUT = [arr(FACE[axis]) for axis, _ in SWAPS]


def swap(x, axis, kind):
    n = lax.axis_size(axis)
    pairs = []
    for i in range(kind, n + kind, 2):
        a, b = i % n, (i + 1) % n
        pairs += [(a, b), (b, a)]
    return lax.ppermute(x, axis, pairs)


def exchange(sends):
    return [swap(s, axis, kind) for s, (axis, kind) in zip(sends, SWAPS)]


def side(axis, kind):
    odd = lax.rem(lax.axis_index(axis), 2)
    return odd if kind else 1 - odd


def face_slices(axis, kind):
    up = side(axis, kind)
    if axis == "gx":
        base = up * ((NX - 1) * PLANE)
        return lambda i: (pl.ds(pl.multiple_of(base + i * NZ, NZ), NZ), pl.ds(pl.multiple_of(i * NZ, NZ), NZ))
    if axis == "gy":
        base = up * ((NY - 1) * NZ)
        return lambda i: (pl.ds(pl.multiple_of(base + i * PLANE, NZ), NZ), pl.ds(pl.multiple_of(i * NZ, NZ), NZ))
    base = up * (NZ - 1)
    return lambda i: (pl.ds(base + i * PLANE, NY, stride=NZ), pl.ds(pl.multiple_of(i * NY, NY), NY))


def loop(n, body, unroll=4):
    def step(i, c):
        body(i)
        return c

    lax.fori_loop(0, n, step, 0, unroll=unroll)


def emit_faces(w, sends):
    for (axis, kind), send in zip(SWAPS, sends):
        at = face_slices(axis, kind)

        def body(i, at=at, send=send):
            src, dst = at(i)
            send[dst, :] = w[src, :]

        loop(NX, body)


def start_kernel(feat, scales, w0, sb, *rest):
    sends, (buf, sems) = rest[:6], rest[6:]

    def copy(i):
        rows = pl.ds(pl.multiple_of(i * PLANE, PLANE), PLANE)
        return pltpu.make_async_copy(feat.at[rows, :], buf.at[rows, :], sems.at[i])

    for i in range(NX):
        copy(i).start()
    for i in range(NX):
        st = jnp.transpose(scales[i], (1, 0))
        copy(i).wait()
        for j in range(NY):
            rows = pl.ds(i * PLANE + j * NZ, NZ)
            b = jnp.broadcast_to(st[:, j : j + 1], (NZ, C))
            sb[rows, :] = b
            w0[rows, :] = b * buf[rows, :]
    emit_faces(w0, sends)


def aux_kernel(sb, weights, a2, rs, w4):
    def body(i):
        rows = pl.ds(pl.multiple_of(i * 64, 64), 64)
        s = sb[rows, :]
        a2[rows, :] = -2.0 * (s * s)
        rs[rows, :] = 1.0 / s

    loop(ROWS // 64, body, 2)
    for layer in range(2):
        w = weights[layer]
        hi = w.astype(jnp.bfloat16)
        lo = (w - hi.astype(F32)).astype(jnp.bfloat16)
        both = jnp.concatenate([hi, lo], axis=1)
        w4[layer, :C, :] = both
        w4[layer, C:, :] = both


def local_kernel(first, *refs):
    if first:
        w, a2, out = refs
        prior = None
    else:
        w, a2, prior, out = refs
    sub = lax.broadcasted_iota(jnp.int32, (8, C), 0)
    top, bottom = sub == 0, sub == 7
    nv = NZ // 8

    def plane(base, lo, hi):
        def at(off):
            return [w[pl.ds(pl.multiple_of(base + off + 8 * k, 8), 8), :] for k in range(nv)]

        below, here = None, at(0)
        for y in range(NY):
            above = at((y + 1) * NZ) if y + 1 < NY else None
            dn = [pltpu.roll(v, 1, 0) for v in here]
            up = [pltpu.roll(v, 7, 0) for v in here]
            low = at(y * NZ - PLANE) if lo else None
            high = at(y * NZ + PLANE) if hi else None
            for k in range(nv):
                n = jnp.where(top, dn[k - 1] if k else 0.0, dn[k]) + jnp.where(
                    bottom, up[k + 1] if k + 1 < nv else 0.0, up[k]
                )
                for other in (below, above, low, high):
                    if other is not None:
                        n = n + other[k]
                rows = pl.ds(pl.multiple_of(base + y * NZ + 8 * k, 8), 8)
                r = a2[rows, :] * n
                out[rows, :] = 0.5 * r if first else r - prior[rows, :]
            below, here = here, above

    plane(0, False, True)
    lax.fori_loop(1, NX - 1, lambda i, c: (plane(pl.multiple_of(i * PLANE, PLANE), True, True), c)[1], 0)
    plane((NX - 1) * PLANE, True, False)


def fix_faces(first, w_in, w, a2, halos):
    for (axis, kind), halo in reversed(list(zip(SWAPS, halos))):
        at = face_slices(axis, kind)

        def body(i, at=at, halo=halo):
            dst, src = at(i)
            r = a2[dst, :] * halo[src, :]
            w[dst, :] = w_in[dst, :] + (0.5 * r if first else r)

        loop(NX, body)


def fix_kernel(first, w_in, a2, *rest):
    halos, w, sends = rest[:6], rest[6], rest[7:]
    fix_faces(first, w, w, a2, halos)
    emit_faces(w, sends)


def mixed(layer, ws, rs, thetas, w4, rows):
    t = None
    for k, w in enumerate(ws):
        term = thetas[layer, k : k + 1, :] * w[rows, :]
        t = term if t is None else t + term
    hi = t.astype(jnp.bfloat16)
    lo = (t - hi.astype(F32)).astype(jnp.bfloat16)
    both = jnp.dot(jnp.concatenate([hi, lo], axis=1), w4[layer], preferred_element_type=F32)
    v = (both[:, :C] + both[:, C:]) * rs[rows, :]
    return v / (1.0 + jnp.exp(-v))


def face_mix_kernel(layer, w0, w1, w2, w3_in, a2, sb, rs, thetas, w4, *rest):
    halos, w3, sends, (ft,) = rest[:6], rest[6], rest[7:13], rest[13:]
    fix_faces(False, w3, w3, a2, halos)
    for (axis, kind), send in zip(SWAPS, sends):
        at = face_slices(axis, kind)
        size = FACE[axis]
        if axis == "gx":
            base = side(axis, kind) * ((NX - 1) * PLANE)

            def body(i, base=base, send=send):
                rows = pl.ds(pl.multiple_of(base + i * 256, 256), 256)
                send[pl.ds(pl.multiple_of(i * 256, 256), 256), :] = sb[rows, :] * mixed(
                    layer, (w0, w1, w2, w3), rs, thetas, w4, rows
                )

            loop(size // 256, body, True)
            continue

        def gather(i, at=at):
            src, dst = at(i)
            for k, w in enumerate((w0, w1, w2, w3, rs, sb)):
                ft[k, dst, :] = w[src, :]

        loop(NX, gather)

        def body(i, send=send):
            rows = pl.ds(pl.multiple_of(i * 256, 256), 256)
            send[rows, :] = ft[5, rows, :] * mixed(
                layer, tuple(ft.at[k] for k in range(4)), ft.at[4], thetas, w4, rows
            )

        loop(size // 256, body, True)


def mix_kernel(layer, w0, w1, w2, w3, sb, rs, thetas, w4, out):
    def body(i):
        rows = pl.ds(pl.multiple_of(i * 256, 256), 256)
        out[rows, :] = sb[rows, :] * mixed(layer, (w0, w1, w2, w3), rs, thetas, w4, rows)

    loop(ROWS // 256, body, 2)


def last_kernel(layer, w0, w1, w2, w3_in, a2, rs, thetas, w4, *rest):
    halos, (w3, out), (buf, sems) = rest[:6], rest[6:8], rest[8:]
    fix_faces(False, w3, w3, a2, halos)

    def copy(i):
        rows = pl.ds(pl.multiple_of(i * PLANE, PLANE), PLANE)
        return pltpu.make_async_copy(buf.at[rows, :], out.at[rows, :], sems.at[i])

    def body(i):
        for h in range(2):
            rows = pl.ds(pl.multiple_of(i * PLANE + h * 256, 256), 256)
            buf[rows, :] = mixed(layer, (w0, w1, w2, w3), rs, thetas, w4, rows)
        copy(i).start()

    loop(NX, body, 1)
    loop(NX, lambda i: copy(i).wait(), 1)


def call(kernel, out_shape, n_in, name, in_hbm=(), out_hbm=(), scratch=(), aliases=None, mib=1):
    return pl.pallas_call(
        kernel,
        out_shape=out_shape,
        in_specs=[HBM if i in in_hbm else VM for i in range(n_in)],
        out_specs=[HBM if i in out_hbm else VM for i in range(len(out_shape))],
        scratch_shapes=list(scratch),
        input_output_aliases=aliases or {},
        compiler_params=pltpu.CompilerParams(vmem_limit_bytes=mib * MIB),
        name=name,
    )


def per_device(features, scales, thetas, weights):
    shape = features.shape
    feat = pltpu.with_memory_space_constraint(features.reshape(ROWS, C), pltpu.HBM)
    dma = [pltpu.VMEM((ROWS, C), F32), pltpu.SemaphoreType.DMA((NX,))]
    w0, sb, *sends = call(
        start_kernel, [arr(ROWS), arr(ROWS)] + FACES_OUT, 2, "start", in_hbm=(0,), scratch=dma, mib=6
    )(feat, scales)
    halos = exchange(sends)
    a2, rs, w4 = call(
        aux_kernel, [arr(ROWS), arr(ROWS), jax.ShapeDtypeStruct((2, 2 * C, 2 * C), jnp.bfloat16)], 2, "aux"
    )(sb, weights)
    for layer in range(2):
        ws = [w0]
        for k in range(1, 4):
            first = k == 1
            prior = [] if first else [ws[-2]]
            (w,) = call(functools.partial(local_kernel, first), [arr(ROWS)], 2 + len(prior), f"local{k}")(
                ws[-1], a2, *prior
            )
            if k < 3:
                w, *sends = call(
                    functools.partial(fix_kernel, first), [arr(ROWS)] + FACES_OUT, 8, f"fix{k}", aliases={0: 0}
                )(w, a2, *halos)
                halos = exchange(sends)
                ws.append(w)
        if layer == 0:
            w, *sends = call(
                functools.partial(face_mix_kernel, layer),
                [arr(ROWS)] + FACES_OUT,
                15,
                "face_mix",
                scratch=[pltpu.VMEM((6, PLANE, C), F32)],
                mib=6,
                aliases={3: 0},
            )(*ws, w, a2, sb, rs, thetas, w4, *halos)
            halos = exchange(sends)
            (w0,) = call(functools.partial(mix_kernel, layer), [arr(ROWS)], 8, "mix")(
                *ws, w, sb, rs, thetas, w4
            )
        else:
            _, out = call(
                functools.partial(last_kernel, layer),
                [arr(ROWS), arr(ROWS)],
                14,
                "last",
                out_hbm=(1,),
                scratch=dma,
                mib=8,
                aliases={3: 0},
            )(*ws, w, a2, rs, thetas, w4, *halos)
    return out.reshape(shape)


def solution(mesh):
    return jax.shard_map(
        per_device,
        mesh=mesh,
        in_specs=(P(*AXES, None), P(*AXES), P(), P()),
        out_specs=P(*AXES, None),
        check_vma=False,
    )
```

```python
import functools

import jax
import jax.numpy as jnp
from jax import lax
from jax.experimental import pallas as pl
from jax.experimental.pallas import tpu as pltpu
from jax.sharding import PartitionSpec as P


AXES = ("gx", "gy", "gz")
NX, NY, NZ, C = 16, 16, 32, 128
PLANE = NY * NZ
ROWS = NX * PLANE
FACE = {"gx": PLANE, "gy": NX * NZ, "gz": NX * NY}
LINE = {"gy": NZ, "gz": NY}
CROSS = ("gx", 1)
LOCALS = (("gy", 0), ("gy", 1), ("gz", 1), ("gz", 0), ("gx", 0))
SCALES = 16

F32 = jnp.float32
VM = pl.BlockSpec(memory_space=pltpu.VMEM)
HBM = pl.BlockSpec(memory_space=pltpu.HBM)
MIB = 1024 * 1024


def arr(rows, cols=C, dtype=F32):
    return jax.ShapeDtypeStruct((rows, cols), dtype)


def locals_out(lines):
    return [arr(FACE[a] + lines * LINE.get(a, 0)) for a, _ in LOCALS]


def swap(x, axis, kind):
    n = lax.axis_size(axis)
    pairs = []
    for i in range(kind, n + kind, 2):
        a, b = i % n, (i + 1) % n
        pairs += [(a, b), (b, a)]
    return lax.ppermute(x, axis, pairs)


def exchange(sends, cross=None, late=None):
    first = [] if cross is None else [swap(cross, *CROSS)]
    got = [swap(s, a, k) for s, (a, k) in zip(sends, LOCALS)]
    last = [] if late is None else [swap(late, *CROSS)]
    return first, got, last


def side(axis, kind):
    odd = lax.rem(lax.axis_index(axis), 2)
    return odd if kind else 1 - odd


def face_slices(axis, kind):
    up = side(axis, kind)
    if axis == "gx":
        base = up * ((NX - 1) * PLANE)
        return lambda i: (pl.ds(pl.multiple_of(base + i * NZ, NZ), NZ), pl.ds(pl.multiple_of(i * NZ, NZ), NZ))
    if axis == "gy":
        base = up * ((NY - 1) * NZ)
        return lambda i: (pl.ds(pl.multiple_of(base + i * PLANE, NZ), NZ), pl.ds(pl.multiple_of(i * NZ, NZ), NZ))
    base = up * (NZ - 1)
    return lambda i: (pl.ds(base + i * PLANE, NY, stride=NZ), pl.ds(pl.multiple_of(i * NY, NY), NY))


def plane_line(axis, kind):
    up = side(axis, kind)
    if axis == "gy":
        return pl.ds(pl.multiple_of(up * ((NY - 1) * NZ), NZ), NZ)
    return pl.ds(up * (NZ - 1), NY, stride=NZ)


def line_rows(axis, i):
    return pl.ds(FACE[axis] + i * LINE[axis], LINE[axis])


def cross_base(depth):
    up = side(*CROSS)
    return pl.multiple_of(up * ((NX - depth) * PLANE) + (1 - up) * ((depth - 1) * PLANE), PLANE)


def loop(n, body, unroll=4):
    def step(i, c):
        body(i)
        return c

    lax.fori_loop(0, n, step, 0, unroll=unroll)


def copy_plane(src, base, dst):
    def body(i):
        at = pl.multiple_of(i * 64, 64)
        dst[pl.ds(at, 64), :] = src[pl.ds(pl.multiple_of(base + at, 64), 64), :]

    loop(PLANE // 64, body)


def emit_face(w, axis, kind, send):
    at = face_slices(axis, kind)

    def body(i):
        src, dst = at(i)
        send[dst, :] = w[src, :]

    loop(NX, body)


def emit_locals(w, sends, ghosts=()):
    for (axis, kind), send in zip(LOCALS, sends):
        emit_face(w, axis, kind, send)
        if axis != "gx":
            for i, g in enumerate(ghosts):
                send[line_rows(axis, i), :] = g[plane_line(axis, kind), :]


def fix_faces(half, w, a2, halos, cross):
    for (axis, kind), halo in list(zip(LOCALS, halos))[::-1] + [(CROSS, cross)]:
        at = face_slices(axis, kind)

        def body(i, at=at, halo=halo):
            dst, src = at(i)
            r = a2[dst, :] * halo[src, :]
            w[dst, :] = w[dst, :] + (0.5 * r if half else r)

        loop(NX, body)


def fix_lines(half, g, a2, halos, i):
    for (axis, kind), halo in zip(LOCALS, halos):
        if axis == "gx":
            continue
        at = plane_line(axis, kind)
        r = a2[at, :] * halo[line_rows(axis, i), :]
        g[at, :] = g[at, :] + (0.5 * r if half else r)


def yz_sums(w, base, emit):
    sub = lax.broadcasted_iota(jnp.int32, (8, C), 0)
    top, bottom = sub == 0, sub == 7
    nv = NZ // 8

    def at(y):
        return [w[pl.ds(pl.multiple_of(base + y * NZ + 8 * k, 8), 8), :] for k in range(nv)]

    below, here = None, at(0)
    for y in range(NY):
        above = at(y + 1) if y + 1 < NY else None
        dn = [pltpu.roll(v, 1, 0) for v in here]
        up = [pltpu.roll(v, 7, 0) for v in here]
        for k in range(nv):
            n = jnp.where(top, dn[k - 1] if k else 0.0, dn[k]) + jnp.where(
                bottom, up[k + 1] if k + 1 < nv else 0.0, up[k]
            )
            for other in (below, above):
                if other is not None:
                    n = n + other[k]
            emit(y * NZ + 8 * k, n)
        below, here = here, above


def rows8(base, r):
    return pl.ds(pl.multiple_of(base + r, 8), 8)


def local_pass(half, w, a2, prior, out):
    def plane(base, lo, hi):
        def emit(r, n):
            if lo:
                n = n + w[rows8(base, r - PLANE), :]
            if hi:
                n = n + w[rows8(base, r + PLANE), :]
            v = a2[rows8(base, r), :] * n
            out[rows8(base, r), :] = 0.5 * v if half else v - prior[rows8(base, r), :]

        yz_sums(w, base, emit)

    plane(0, False, True)
    lax.fori_loop(1, NX - 1, lambda i, c: (plane(pl.multiple_of(i * PLANE, PLANE), True, True), c)[1], 0)
    plane((NX - 1) * PLANE, True, False)


def ghost_pass(half, g, inner, inner_base, a2, prior, out):
    def emit(r, n):
        v = a2[rows8(0, r), :] * (n + inner[rows8(inner_base, r), :])
        out[rows8(0, r), :] = 0.5 * v if half else v - prior[rows8(0, r), :]

    yz_sums(g, 0, emit)


def ghost_add(half, g, a2, outer, out):
    def body(i):
        rows = pl.ds(pl.multiple_of(i * 64, 64), 64)
        r = a2[rows, :] * outer[rows, :]
        out[rows, :] = g[rows, :] + (0.5 * r if half else r)

    loop(PLANE // 64, body)


def spread(tile, emit):
    st = jnp.transpose(tile, (1, 0))
    for j in range(NY):
        emit(j, jnp.broadcast_to(st[:NZ, j : j + 1], (NZ, C)))


def start_kernel(feat, scales, w0, sb, d1, d2, d3, *rest):
    sends, (buf, sems) = rest[:5], rest[5:]

    def copy(i):
        rows = pl.ds(pl.multiple_of(i * PLANE, PLANE), PLANE)
        return pltpu.make_async_copy(feat.at[rows, :], buf.at[rows, :], sems.at[i])

    for i in range(NX):
        copy(i).start()
    for i in range(NX):
        copy(i).wait()

        def emit(j, b, i=i):
            rows = pl.ds(i * PLANE + j * NZ, NZ)
            sb[rows, :] = b
            w0[rows, :] = b * buf[rows, :]

        spread(scales[i], emit)
    up = side(*CROSS)
    for depth, d in ((1, d1), (2, d2), (3, d3)):
        copy_plane(w0, cross_base(depth), d)
        if depth < 3:
            d[PLANE:, :] = jnp.zeros((SCALES, C), F32)
            d[PLANE:, :NZ] = scales[up * (NX - depth) + (1 - up) * (depth - 1)]
    emit_locals(w0, sends)


def aux_kernel(sb, weights, a2, rs, w4):
    def body(i):
        rows = pl.ds(pl.multiple_of(i * 64, 64), 64)
        s = sb[rows, :]
        a2[rows, :] = -2.0 * (s * s)
        rs[rows, :] = 1.0 / s

    loop(ROWS // 64, body, 2)
    for layer in range(2):
        w = weights[layer]
        hi = w.astype(jnp.bfloat16)
        lo = (w - hi.astype(F32)).astype(jnp.bfloat16)
        both = jnp.concatenate([hi, lo], axis=1)
        w4[layer, :C, :] = both
        w4[layer, C:, :] = both


def ghost_aux_kernel(d, a2g):
    def emit(j, b):
        a2g[pl.ds(j * NZ, NZ), :] = -2.0 * (b * b)

    spread(d[PLANE:, :], emit)


def local1_kernel(w0, a2, w1):
    local_pass(True, w0, a2, None, w1)


def local2_kernel(w1, a2, w0, d1, a2g1, w2, p1):
    local_pass(False, w1, a2, w0, w2)
    ghost_pass(True, d1, w0, cross_base(1), a2g1, None, p1)


def local3_kernel(w2, a2, w1, d1, d2, w1g1, a2g1, a2g2, w3, p2, q1):
    local_pass(False, w2, a2, w1, w3)
    ghost_pass(True, d2, d1, 0, a2g2, None, p2)
    ghost_pass(False, w1g1, w1, cross_base(1), a2g1, d1, q1)


def fix1_kernel(w_in, a2, d1, *rest):
    halos, w, sends = rest[:5], rest[5], rest[6:]
    fix_faces(True, w, a2, halos, d1)
    emit_locals(w, sends, (d1,))


def fix2_kernel(w_in, a2, d2, p1, a2g1, *rest):
    halos, w, w1g1, sends = rest[:5], rest[5], rest[6], rest[7:]
    ghost_add(True, p1, a2g1, d2, w1g1)
    fix_lines(True, w1g1, a2g1, halos, 0)
    fix_faces(False, w, a2, halos, w1g1)
    emit_locals(w, sends, (w1g1, d2))


def fix3(w, a2, d3, p2, q1, a2g1, a2g2, halos, g2, g1):
    ghost_add(True, p2, a2g2, d3, g2)
    fix_lines(True, g2, a2g2, halos, 1)
    ghost_add(False, q1, a2g1, g2, g1)
    fix_lines(False, g1, a2g1, halos, 0)
    fix_faces(False, w, a2, halos, g1)


def mixed(layer, ws, rs, thetas, w4, rows):
    t = None
    for k, w in enumerate(ws):
        term = thetas[layer, k : k + 1, :] * w[rows, :]
        t = term if t is None else t + term
    hi = t.astype(jnp.bfloat16)
    lo = (t - hi.astype(F32)).astype(jnp.bfloat16)
    both = jnp.dot(jnp.concatenate([hi, lo], axis=1), w4[layer], preferred_element_type=F32)
    v = (both[:, :C] + both[:, C:]) * rs[rows, :]
    return v / (1.0 + jnp.exp(-v))


def face_mix_kernel(layer, w3_in, a2, d3, p2, q1, a2g1, a2g2, w0, w1, w2, sb, rs, thetas, w4, *rest):
    halos, w3, d1, sends, (g2, g1, ft) = rest[:5], rest[5], rest[6], rest[7:12], rest[12:]
    fix3(w3, a2, d3, p2, q1, a2g1, a2g2, halos, g2, g1)
    ws = (w0, w1, w2, w3)
    for (axis, kind), send in [(CROSS, d1)] + list(zip(LOCALS, sends)):
        at = face_slices(axis, kind)
        size = FACE[axis]
        if axis == "gx":
            base = side(axis, kind) * ((NX - 1) * PLANE)

            def body(i, base=base, send=send):
                rows = pl.ds(pl.multiple_of(base + i * 256, 256), 256)
                send[pl.ds(pl.multiple_of(i * 256, 256), 256), :] = sb[rows, :] * mixed(
                    layer, ws, rs, thetas, w4, rows
                )

            loop(size // 256, body, True)
            continue

        def gather(i, at=at):
            src, dst = at(i)
            for k, w in enumerate(ws + (rs, sb)):
                ft[k, dst, :] = w[src, :]

        loop(NX, gather)

        def body(i, send=send):
            rows = pl.ds(pl.multiple_of(i * 256, 256), 256)
            send[rows, :] = ft[5, rows, :] * mixed(
                layer, tuple(ft.at[k] for k in range(4)), ft.at[4], thetas, w4, rows
            )

        loop(size // 256, body, True)


def mix_kernel(layer, w0, w1, w2, w3, sb, rs, thetas, w4, out, d2, d3):
    def body(i):
        rows = pl.ds(pl.multiple_of(i * 256, 256), 256)
        out[rows, :] = sb[rows, :] * mixed(layer, (w0, w1, w2, w3), rs, thetas, w4, rows)

    loop(ROWS // 256, body, 2)
    copy_plane(out, cross_base(2), d2)
    copy_plane(out, cross_base(3), d3)


def last_kernel(layer, w3_in, a2, d3, p2, q1, a2g1, a2g2, w0, w1, w2, rs, thetas, w4, *rest):
    halos, (w3, out), (g2, g1, buf, sems) = rest[:5], rest[5:7], rest[7:]
    fix3(w3, a2, d3, p2, q1, a2g1, a2g2, halos, g2, g1)

    def copy(i):
        rows = pl.ds(pl.multiple_of(i * PLANE, PLANE), PLANE)
        return pltpu.make_async_copy(buf.at[rows, :], out.at[rows, :], sems.at[i])

    def body(i):
        for h in range(2):
            rows = pl.ds(pl.multiple_of(i * PLANE + h * 256, 256), 256)
            buf[rows, :] = mixed(layer, (w0, w1, w2, w3), rs, thetas, w4, rows)
        copy(i).start()

    loop(NX, body, 1)
    loop(NX, lambda i: copy(i).wait(), 1)


def call(kernel, out_shape, args, in_hbm=(), out_hbm=(), scratch=(), aliases=None, mib=1):
    return pl.pallas_call(
        kernel,
        out_shape=out_shape,
        in_specs=[HBM if i in in_hbm else VM for i in range(len(args))],
        out_specs=[HBM if i in out_hbm else VM for i in range(len(out_shape))],
        scratch_shapes=list(scratch),
        input_output_aliases=aliases or {},
        compiler_params=pltpu.CompilerParams(vmem_limit_bytes=mib * MIB),
    )(*args)


def per_device(features, scales, thetas, weights):
    shape = features.shape
    feat = pltpu.with_memory_space_constraint(features.reshape(ROWS, C), pltpu.HBM)
    block, plane = arr(ROWS), arr(PLANE)
    dma = [pltpu.VMEM((ROWS, C), F32), pltpu.SemaphoreType.DMA((NX,))]
    ghosts = [pltpu.VMEM((PLANE, C), F32)] * 2
    w0, sb, s1, s2, s3, *sends = call(
        start_kernel,
        [block, block, arr(PLANE + SCALES), arr(PLANE + SCALES), plane] + locals_out(0),
        (feat, scales),
        in_hbm=(0,),
        scratch=dma,
        mib=6,
    )
    for layer in range(2):
        last = layer == 1
        if last:
            w0, s2, s3 = call(
                functools.partial(mix_kernel, 0), [block, plane, plane], (w0, w1, w2, w3, sb, rs, thetas, w4)
            )
        (d1,), halos, (d2,) = exchange(sends, cross=s1, late=s2)
        if not last:
            a2, rs, w4 = call(
                aux_kernel, [block, block, jax.ShapeDtypeStruct((2, 2 * C, 2 * C), jnp.bfloat16)], (sb, weights)
            )
        (w1,) = call(local1_kernel, [block], (w0, a2))
        w1, *sends = call(fix1_kernel, [block] + locals_out(1), (w1, a2, d1, *halos), aliases={0: 0})
        _, halos, (d3,) = exchange(sends, late=s3)
        if not last:
            (a2g1,) = call(ghost_aux_kernel, [plane], (d1,))
        w2, p1 = call(local2_kernel, [block, plane], (w1, a2, w0, d1, a2g1))
        w2, w1g1, *sends = call(
            fix2_kernel, [block, plane] + locals_out(2), (w2, a2, d2, p1, a2g1, *halos), aliases={0: 0}
        )
        _, halos, _ = exchange(sends)
        if not last:
            (a2g2,) = call(ghost_aux_kernel, [plane], (d2,))
        w3, p2, q1 = call(local3_kernel, [block, plane, plane], (w2, a2, w1, d1, d2, w1g1, a2g1, a2g2))
        tail = (w3, a2, d3, p2, q1, a2g1, a2g2, w0, w1, w2)
        if not last:
            w3, s1, *sends = call(
                functools.partial(face_mix_kernel, layer),
                [block, plane] + locals_out(0),
                (*tail, sb, rs, thetas, w4, *halos),
                scratch=ghosts + [pltpu.VMEM((6, PLANE, C), F32)],
                mib=6,
                aliases={0: 0},
            )
        else:
            _, out = call(
                functools.partial(last_kernel, layer),
                [block, block],
                (*tail, rs, thetas, w4, *halos),
                out_hbm=(1,),
                scratch=ghosts + dma,
                mib=8,
                aliases={0: 0},
            )
    return out.reshape(shape)


def solution(mesh):
    return jax.shard_map(
        per_device,
        mesh=mesh,
        in_specs=(P(*AXES, None), P(*AXES), P(), P()),
        out_specs=P(*AXES, None),
        check_vma=False,
    )
```

```python
import functools

import jax
import jax.numpy as jnp
from jax import lax
from jax.experimental import pallas as pl
from jax.experimental.pallas import tpu as pltpu
from jax.sharding import PartitionSpec as P


AXES = ("gx", "gy", "gz")
NX, NY, NZ, C = 16, 16, 32, 128
PLANE = NY * NZ
ROWS = NX * PLANE
FACE = {"gx": PLANE, "gy": NX * NZ, "gz": NX * NY}
LINE = {"gy": NZ, "gz": NY}
CROSS = ("gx", 1)
LOCALS = (("gy", 0), ("gy", 1), ("gz", 1), ("gz", 0), ("gx", 0))
FACE_ROWS = 2 * (FACE["gy"] + FACE["gz"])
SCALES = 16

F32 = jnp.float32
VM = pl.BlockSpec(memory_space=pltpu.VMEM)
HBM = pl.BlockSpec(memory_space=pltpu.HBM)
MIB = 1024 * 1024


def arr(rows, cols=C, dtype=F32):
    return jax.ShapeDtypeStruct((rows, cols), dtype)


def locals_out(lines):
    return [arr(FACE[a] + lines * LINE.get(a, 0)) for a, _ in LOCALS]


def swap(x, axis, kind):
    n = lax.axis_size(axis)
    pairs = []
    for i in range(kind, n + kind, 2):
        a, b = i % n, (i + 1) % n
        pairs += [(a, b), (b, a)]
    return lax.ppermute(x, axis, pairs)


def exchange(sends, cross=None, late=None):
    first = [] if cross is None else [swap(cross, *CROSS)]
    got = [swap(s, a, k) for s, (a, k) in zip(sends, LOCALS)]
    last = [] if late is None else [swap(late, *CROSS)]
    return first, got, last


def side(axis, kind):
    odd = lax.rem(lax.axis_index(axis), 2)
    return odd if kind else 1 - odd


def face_slices(axis, kind):
    up = side(axis, kind)
    if axis == "gx":
        base = up * ((NX - 1) * PLANE)
        return lambda i: (pl.ds(pl.multiple_of(base + i * NZ, NZ), NZ), pl.ds(pl.multiple_of(i * NZ, NZ), NZ))
    if axis == "gy":
        base = up * ((NY - 1) * NZ)
        return lambda i: (pl.ds(pl.multiple_of(base + i * PLANE, NZ), NZ), pl.ds(pl.multiple_of(i * NZ, NZ), NZ))
    base = up * (NZ - 1)
    return lambda i: (pl.ds(base + i * PLANE, NY, stride=NZ), pl.ds(pl.multiple_of(i * NY, NY), NY))


def plane_line(axis, kind):
    up = side(axis, kind)
    if axis == "gy":
        return pl.ds(pl.multiple_of(up * ((NY - 1) * NZ), NZ), NZ)
    return pl.ds(up * (NZ - 1), NY, stride=NZ)


def line_rows(axis, i):
    return pl.ds(FACE[axis] + i * LINE[axis], LINE[axis])


def cross_base(depth):
    up = side(*CROSS)
    return pl.multiple_of(up * ((NX - depth) * PLANE) + (1 - up) * ((depth - 1) * PLANE), PLANE)


def loop(n, body, unroll=4):
    def step(i, c):
        body(i)
        return c

    lax.fori_loop(0, n, step, 0, unroll=unroll)


def copy_plane(src, base, dst):
    for i in range(PLANE // 128):
        rows = pl.ds(i * 128, 128)
        dst[rows, :] = src[pl.ds(pl.multiple_of(base + i * 128, 128), 128), :]


def batches(axis):
    size = 8 if axis == "gz" else 4
    return [range(g, g + size) for g in range(0, NX, size)]


def emit_face(w, axis, kind, send, only=None):
    at = face_slices(axis, kind)
    for group in batches(axis) if only is None else [only]:
        got = [w[at(i)[0], :] for i in group]
        for i, v in zip(group, got):
            send[at(i)[1], :] = v


def fix_faces(half, w, a2, halos, cross, sends=None):
    todo = [(a, k, h, None if sends is None else s) for (a, k), h, s in zip(LOCALS, halos, sends or [None] * 5)]
    order = [t for t in todo if t[0] == "gz"] + [t for t in todo if t[0] == "gy"]
    for axis, kind, halo, send in order + [(*CROSS, cross, None), todo[-1]]:
        at = face_slices(axis, kind)
        for group in batches(axis):
            got = []
            for i in group:
                dst, src = at(i)
                r = a2[dst, :] * halo[src, :]
                got.append(w[dst, :] + (0.5 * r if half else r))
            for i, v in zip(group, got):
                w[at(i)[0], :] = v
                if send is not None and axis != "gz":
                    send[at(i)[1], :] = v
    for axis, kind, _, send in order if sends else ():
        emit_face(w, axis, kind, send, (0, NX - 1) if axis == "gy" else None)


def emit_ghost_lines(ghosts, sends):
    for (axis, kind), send in zip(LOCALS, sends):
        if axis != "gx":
            for i, g in enumerate(ghosts):
                send[line_rows(axis, i), :] = g[plane_line(axis, kind), :]


def fix_lines(half, g, a2, halos, i):
    for (axis, kind), halo in zip(LOCALS, halos):
        if axis == "gx":
            continue
        at = plane_line(axis, kind)
        r = a2[at, :] * halo[line_rows(axis, i), :]
        g[at, :] = g[at, :] + (0.5 * r if half else r)


def yz_sums(w, base, emit):
    sub = lax.broadcasted_iota(jnp.int32, (8, C), 0)
    top, bottom = sub == 0, sub == 7
    nv = NZ // 8

    def at(y):
        return [w[pl.ds(pl.multiple_of(base + y * NZ + 8 * k, 8), 8), :] for k in range(nv)]

    below, here = None, at(0)
    for y in range(NY):
        above = at(y + 1) if y + 1 < NY else None
        dn = [pltpu.roll(v, 1, 0) for v in here]
        up = [pltpu.roll(v, 7, 0) for v in here]
        for k in range(nv):
            n = jnp.where(top, dn[k - 1] if k else 0.0, dn[k]) + jnp.where(
                bottom, up[k + 1] if k + 1 < nv else 0.0, up[k]
            )
            for other in (below, above):
                if other is not None:
                    n = n + other[k]
            emit(y * NZ + 8 * k, n)
        below, here = here, above


def rows8(base, r):
    return pl.ds(pl.multiple_of(base + r, 8), 8)


def local_pass(half, w, a2, prior, out):
    def plane(base, lo, hi):
        def emit(r, n):
            if lo:
                n = n + w[rows8(base, r - PLANE), :]
            if hi:
                n = n + w[rows8(base, r + PLANE), :]
            v = a2[rows8(base, r), :] * n
            out[rows8(base, r), :] = 0.5 * v if half else v - prior[rows8(base, r), :]

        yz_sums(w, base, emit)

    plane(0, False, True)
    lax.fori_loop(1, NX - 1, lambda i, c: (plane(pl.multiple_of(i * PLANE, PLANE), True, True), c)[1], 0)
    plane((NX - 1) * PLANE, True, False)


def ghost_pass(half, g, inner, inner_base, a2, prior, out):
    def emit(r, n):
        v = a2[rows8(0, r), :] * (n + inner[rows8(inner_base, r), :])
        out[rows8(0, r), :] = 0.5 * v if half else v - prior[rows8(0, r), :]

    yz_sums(g, 0, emit)


def ghost_add(half, g, a2, outer, out):
    def body(i):
        rows = pl.ds(pl.multiple_of(i * 64, 64), 64)
        r = a2[rows, :] * outer[rows, :]
        out[rows, :] = g[rows, :] + (0.5 * r if half else r)

    loop(PLANE // 64, body)


def spread(tile, emit):
    st = jnp.transpose(tile, (1, 0))
    for j in range(NY):
        emit(j, jnp.broadcast_to(st[:NZ, j : j + 1], (NZ, C)))


def start_kernel(feat, scales, fv, sb, d1, d2, d3, *rest):
    sends, (sv, sems) = rest[:5], rest[5:]
    first = pltpu.make_async_copy(scales, sv, sems.at[NX])
    first.start()

    def copy(i):
        rows = pl.ds(i * PLANE, PLANE)
        return pltpu.make_async_copy(feat.at[rows, :], fv.at[rows, :], sems.at[i])

    for i in range(NX):
        copy(i).start()
    first.wait()
    for i in range(NX):

        def emit(j, b, i=i):
            sb[pl.ds(i * PLANE + j * NZ, NZ), :] = b

        spread(sv[i], emit)
    for i in range(NX):
        copy(i).wait()
    up = side(*CROSS)
    for depth, d in ((1, d1), (2, d2), (3, d3)):
        base = cross_base(depth)
        for i in range(PLANE // 128):
            rows = pl.ds(pl.multiple_of(base + i * 128, 128), 128)
            d[pl.ds(i * 128, 128), :] = sb[rows, :] * fv[rows, :]
        if depth < 3:
            d[PLANE:, :] = jnp.zeros((SCALES, C), F32)
            d[PLANE:, :NZ] = sv[up * (NX - depth) + (1 - up) * (depth - 1)]
    for (axis, kind), send in zip(LOCALS, sends):
        at = face_slices(axis, kind)
        for group in batches(axis):
            got = [sb[at(i)[0], :] * fv[at(i)[0], :] for i in group]
            for i, v in zip(group, got):
                send[at(i)[1], :] = v


def aux_kernel(sb, fv, weights, w0, a2, w4):
    def body(i):
        rows = pl.ds(pl.multiple_of(i * 128, 128), 128)
        s = sb[rows, :]
        w0[rows, :] = s * fv[rows, :]
        a2[rows, :] = -2.0 * (s * s)

    loop(ROWS // 128, body, 1)
    for layer in range(2):
        w = weights[layer]
        hi = w.astype(jnp.bfloat16)
        lo = (w - hi.astype(F32)).astype(jnp.bfloat16)
        both = jnp.concatenate([hi, lo], axis=1)
        w4[layer, :C, :] = both
        w4[layer, C:, :] = both


def ghost_aux_kernel(d, a2g):
    def emit(j, b):
        a2g[pl.ds(j * NZ, NZ), :] = -2.0 * (b * b)

    spread(d[PLANE:, :], emit)


def local1_kernel(w0, a2, w1):
    local_pass(True, w0, a2, None, w1)


def local2_kernel(w1, a2, w0, d1, a2g1, w2, p1):
    local_pass(False, w1, a2, w0, w2)
    ghost_pass(True, d1, w0, cross_base(1), a2g1, None, p1)


def local3_kernel(w2, a2, w1, d1, d2, w1g1, a2g1, a2g2, w3, p2, q1):
    local_pass(False, w2, a2, w1, w3)
    ghost_pass(True, d2, d1, 0, a2g2, None, p2)
    ghost_pass(False, w1g1, w1, cross_base(1), a2g1, d1, q1)


def fix1_kernel(w_in, a2, d1, *rest):
    halos, w, sends = rest[:5], rest[5], rest[6:]
    fix_faces(True, w, a2, halos, d1, sends)
    emit_ghost_lines((d1,), sends)


def fix2_kernel(w_in, a2, d2, p1, a2g1, *rest):
    halos, w, w1g1, sends = rest[:5], rest[5], rest[6], rest[7:]
    ghost_add(True, p1, a2g1, d2, w1g1)
    fix_lines(True, w1g1, a2g1, halos, 0)
    fix_faces(False, w, a2, halos, w1g1, sends)
    emit_ghost_lines((w1g1, d2), sends)


def fix3(w, a2, d3, p2, q1, a2g1, a2g2, halos, g2, g1):
    ghost_add(True, p2, a2g2, d3, g2)
    fix_lines(True, g2, a2g2, halos, 1)
    ghost_add(False, q1, a2g1, g2, g1)
    fix_lines(False, g1, a2g1, halos, 0)
    fix_faces(False, w, a2, halos, g1)


def mixed(layer, ws, a2, thetas, w4, rows, scaled):
    t = None
    for k, w in enumerate(ws):
        term = thetas[layer, k : k + 1, :] * w[rows, :]
        t = term if t is None else t + term
    hi = t.astype(jnp.bfloat16)
    lo = (t - hi.astype(F32)).astype(jnp.bfloat16)
    both = jnp.dot(jnp.concatenate([hi, lo], axis=1), w4[layer], preferred_element_type=F32)
    q = -0.5 * a2[rows, :]
    r = lax.rsqrt(q)
    h = (both[:, :C] + both[:, C:]) * (0.5 * r)
    out = h + h * jnp.tanh(h)
    return (q * r) * out if scaled else out


def face_mix_kernel(layer, w3_in, a2, d3, p2, q1, a2g1, a2g2, w0, w1, w2, thetas, w4, *rest):
    halos, w3, d1, sends, (g2, g1, ft) = rest[:5], rest[5], rest[6], rest[7:12], rest[12:]
    fix3(w3, a2, d3, p2, q1, a2g1, a2g2, halos, g2, g1)
    ws = (w0, w1, w2, w3)
    at_row = 0
    for (axis, kind), send in zip(LOCALS, sends):
        if axis == "gx":
            continue
        at = face_slices(axis, kind)
        for group in batches(axis):
            for k, w in enumerate(ws + (a2,)):
                got = [w[at(i)[0], :] for i in group]
                for i, v in zip(group, got):
                    ft[k, pl.ds(at_row + i * LINE[axis], LINE[axis]), :] = v
        at_row += FACE[axis]
    for axis, kind, send in ((*CROSS, d1), (*LOCALS[-1], sends[-1])):
        base = side(axis, kind) * ((NX - 1) * PLANE)
        for i in range(PLANE // 256):
            rows = pl.ds(pl.multiple_of(base + i * 256, 256), 256)
            send[pl.ds(i * 256, 256), :] = mixed(layer, ws, a2, thetas, w4, rows, True)
    at_row = 0
    fts = tuple(ft.at[k] for k in range(4))
    for (axis, kind), send in zip(LOCALS[:-1], sends):
        for i in range(FACE[axis] // 256):
            rows = pl.ds(at_row + i * 256, 256)
            send[pl.ds(i * 256, 256), :] = mixed(layer, fts, ft.at[4], thetas, w4, rows, True)
        at_row += FACE[axis]


def mix_kernel(layer, w0, w1, w2, w3, a2, thetas, w4, out, d2, d3):
    def body(i):
        rows = pl.ds(pl.multiple_of(i * 256, 256), 256)
        out[rows, :] = mixed(layer, (w0, w1, w2, w3), a2, thetas, w4, rows, True)

    loop(ROWS // 256, body, 4)
    copy_plane(out, cross_base(2), d2)
    copy_plane(out, cross_base(3), d3)


def last_kernel(layer, w3_in, a2, d3, p2, q1, a2g1, a2g2, w0, w1, w2, thetas, w4, *rest):
    halos, (w3, out), (g2, g1, buf, sems) = rest[:5], rest[5:7], rest[7:]
    fix3(w3, a2, d3, p2, q1, a2g1, a2g2, halos, g2, g1)
    step = 1024

    def copy(i):
        rows = pl.ds(pl.multiple_of(i * step, step), step)
        return pltpu.make_async_copy(buf.at[rows, :], out.at[rows, :], sems.at[i])

    def body(i):
        for h in range(step // 256):
            rows = pl.ds(pl.multiple_of(i * step + h * 256, 256), 256)
            buf[rows, :] = mixed(layer, (w0, w1, w2, w3), a2, thetas, w4, rows, False)
        copy(i).start()

    loop(ROWS // step, body, 1)
    loop(ROWS // step, lambda i: copy(i).wait(), 1)


def call(kernel, out_shape, args, in_hbm=(), out_hbm=(), scratch=(), aliases=None, mib=1):
    return pl.pallas_call(
        kernel,
        out_shape=out_shape,
        in_specs=[HBM if i in in_hbm else VM for i in range(len(args))],
        out_specs=[HBM if i in out_hbm else VM for i in range(len(out_shape))],
        scratch_shapes=list(scratch),
        input_output_aliases=aliases or {},
        compiler_params=pltpu.CompilerParams(vmem_limit_bytes=mib * MIB),
    )(*args)


def per_device(features, scales, thetas, weights):
    shape = features.shape
    feat = pltpu.with_memory_space_constraint(features.reshape(ROWS, C), pltpu.HBM)
    block, plane = arr(ROWS), arr(PLANE)
    scales = pltpu.with_memory_space_constraint(scales, pltpu.HBM)
    ghosts = [pltpu.VMEM((PLANE, C), F32)] * 2
    fv, sb, s1, s2, s3, *sends = call(
        start_kernel,
        [block, block, arr(PLANE + SCALES), arr(PLANE + SCALES), plane] + locals_out(0),
        (feat, scales),
        in_hbm=(0, 1),
        scratch=[pltpu.VMEM(scales.shape, F32), pltpu.SemaphoreType.DMA((NX + 1,))],
    )
    for layer in range(2):
        last = layer == 1
        if last:
            w0, s2, s3 = call(functools.partial(mix_kernel, 0), [block, plane, plane], (w0, w1, w2, w3, a2, thetas, w4))
        (d1,), halos, (d2,) = exchange(sends, cross=s1, late=s2)
        if not last:
            w4 = jax.ShapeDtypeStruct((2, 2 * C, 2 * C), jnp.bfloat16)
            w0, a2, w4 = call(aux_kernel, [block, block, w4], (sb, fv, weights))
        (w1,) = call(local1_kernel, [block], (w0, a2))
        w1, *sends = call(fix1_kernel, [block] + locals_out(1), (w1, a2, d1, *halos), aliases={0: 0})
        _, halos, (d3,) = exchange(sends, late=s3)
        if not last:
            (a2g1,) = call(ghost_aux_kernel, [plane], (d1,))
        w2, p1 = call(local2_kernel, [block, plane], (w1, a2, w0, d1, a2g1))
        w2, w1g1, *sends = call(
            fix2_kernel, [block, plane] + locals_out(2), (w2, a2, d2, p1, a2g1, *halos), aliases={0: 0}
        )
        _, halos, _ = exchange(sends)
        if not last:
            (a2g2,) = call(ghost_aux_kernel, [plane], (d2,))
        w3, p2, q1 = call(local3_kernel, [block, plane, plane], (w2, a2, w1, d1, d2, w1g1, a2g1, a2g2))
        tail = (w3, a2, d3, p2, q1, a2g1, a2g2, w0, w1, w2)
        if not last:
            w3, s1, *sends = call(
                functools.partial(face_mix_kernel, layer),
                [block, plane] + locals_out(0),
                (*tail, thetas, w4, *halos),
                scratch=ghosts + [pltpu.VMEM((5, FACE_ROWS, C), F32)],
                mib=7,
                aliases={0: 0},
            )
        else:
            _, out = call(
                functools.partial(last_kernel, layer),
                [block, block],
                (*tail, thetas, w4, *halos),
                out_hbm=(1,),
                scratch=ghosts + [pltpu.VMEM((ROWS, C), F32), pltpu.SemaphoreType.DMA((8,))],
                mib=8,
                aliases={0: 0},
            )
    return out.reshape(shape)


def solution(mesh):
    return jax.shard_map(
        per_device,
        mesh=mesh,
        in_specs=(P(*AXES, None), P(*AXES), P(), P()),
        out_specs=P(*AXES, None),
        check_vma=False,
    )
```

```python
import functools

import jax
import jax.numpy as jnp
from jax import lax
from jax.experimental import pallas as pl
from jax.experimental.pallas import tpu as pltpu
from jax.sharding import PartitionSpec as P


AXES = ("gx", "gy", "gz")
NX, NY, NZ, C = 16, 16, 32, 128
PLANE = NY * NZ
ROWS = NX * PLANE
FACE = {"gx": PLANE, "gy": NX * NZ, "gz": NX * NY}
LINE = {"gy": NZ, "gz": NY}
CROSS = ("gx", 1)
LOCALS = (("gy", 0), ("gy", 1), ("gz", 1), ("gz", 0), ("gx", 0))
SCALES = 16

F32 = jnp.float32
VM = pl.BlockSpec(memory_space=pltpu.VMEM)
HBM = pl.BlockSpec(memory_space=pltpu.HBM)
MIB = 1024 * 1024


def arr(rows, cols=C, dtype=F32):
    return jax.ShapeDtypeStruct((rows, cols), dtype)


def locals_out(lines):
    return [arr(FACE[a] + lines * LINE.get(a, 0)) for a, _ in LOCALS]


def swap(x, axis, kind):
    n = lax.axis_size(axis)
    pairs = []
    for i in range(kind, n + kind, 2):
        a, b = i % n, (i + 1) % n
        pairs += [(a, b), (b, a)]
    return lax.ppermute(x, axis, pairs)


def exchange(sends, cross=None, late=None):
    first = [] if cross is None else [swap(cross, *CROSS)]
    got = [swap(s, a, k) for s, (a, k) in zip(sends, LOCALS)]
    last = [] if late is None else [swap(late, *CROSS)]
    return first, got, last


def side(axis, kind):
    odd = lax.rem(lax.axis_index(axis), 2)
    return odd if kind else 1 - odd


def face_slices(axis, kind):
    up = side(axis, kind)
    if axis == "gx":
        base = up * ((NX - 1) * PLANE)
        return lambda i: (pl.ds(pl.multiple_of(base + i * NZ, NZ), NZ), pl.ds(pl.multiple_of(i * NZ, NZ), NZ))
    if axis == "gy":
        base = up * ((NY - 1) * NZ)
        return lambda i: (pl.ds(pl.multiple_of(base + i * PLANE, NZ), NZ), pl.ds(pl.multiple_of(i * NZ, NZ), NZ))
    base = up * (NZ - 1)
    return lambda i: (pl.ds(base + i * PLANE, NY, stride=NZ), pl.ds(pl.multiple_of(i * NY, NY), NY))


def plane_line(axis, kind):
    up = side(axis, kind)
    if axis == "gy":
        return pl.ds(pl.multiple_of(up * ((NY - 1) * NZ), NZ), NZ)
    return pl.ds(up * (NZ - 1), NY, stride=NZ)


def line_rows(axis, i):
    return pl.ds(FACE[axis] + i * LINE[axis], LINE[axis])


def cross_base(depth):
    up = side(*CROSS)
    return pl.multiple_of(up * ((NX - depth) * PLANE) + (1 - up) * ((depth - 1) * PLANE), PLANE)


def loop(n, body, unroll=4):
    def step(i, c):
        body(i)
        return c

    lax.fori_loop(0, n, step, 0, unroll=unroll)


def copy_plane(src, base, dst):
    for i in range(PLANE // 128):
        rows = pl.ds(i * 128, 128)
        dst[rows, :] = src[pl.ds(pl.multiple_of(base + i * 128, 128), 128), :]


def batches(axis):
    size = 8 if axis == "gz" else 4
    return [range(g, g + size) for g in range(0, NX, size)]


def emit_face(w, axis, kind, send):
    at = face_slices(axis, kind)
    for group in batches(axis):
        got = [w[at(i)[0], :] for i in group]
        for i, v in zip(group, got):
            send[at(i)[1], :] = v


def fix_faces(half, w, a2, zfaces, halos, cross, sends):
    local = list(zip(LOCALS, halos, sends))
    plain = [(CROSS, cross)] + [(k, h) for k, h, _ in local if k[0] == "gx"] + [(k, h) for k, h, _ in local if k[0] == "gy"]
    for key, halo in plain:
        at = face_slices(*key)
        for group in batches(key[0]):
            got = []
            for i in group:
                dst, src = at(i)
                r = a2[dst, :] * halo[src, :]
                got.append(w[dst, :] + (0.5 * r if half else r))
            for i, v in zip(group, got):
                w[at(i)[0], :] = v
    for ((key, halo, send), face) in zip([t for t in local if t[0][0] == "gz"], zfaces):
        at = face_slices(*key)
        for group in batches("gz"):
            got = []
            for i in group:
                dst, src = at(i)
                r = face[src, :] * halo[src, :]
                got.append(w[dst, :] + (0.5 * r if half else r))
            for i, v in zip(group, got):
                w[at(i)[0], :] = v
                send[at(i)[1], :] = v
    for (axis, kind), _, send in local:
        if axis != "gz" and send is not None:
            emit_face(w, axis, kind, send)


def emit_ghost_lines(ghosts, sends):
    for (axis, kind), send in zip(LOCALS, sends):
        if axis != "gx":
            for i, g in enumerate(ghosts):
                send[line_rows(axis, i), :] = g[plane_line(axis, kind), :]


def fix_lines(half, g, a2, halos, i):
    for (axis, kind), halo in zip(LOCALS, halos):
        if axis == "gx":
            continue
        at = plane_line(axis, kind)
        r = a2[at, :] * halo[line_rows(axis, i), :]
        g[at, :] = g[at, :] + (0.5 * r if half else r)


def yz_sums(w, base, emit):
    sub = lax.broadcasted_iota(jnp.int32, (8, C), 0)
    top, bottom = sub == 0, sub == 7
    nv = NZ // 8

    def at(y):
        return [w[pl.ds(pl.multiple_of(base + y * NZ + 8 * k, 8), 8), :] for k in range(nv)]

    below, here = None, at(0)
    for y in range(NY):
        above = at(y + 1) if y + 1 < NY else None
        dn = [pltpu.roll(v, 1, 0) for v in here]
        up = [pltpu.roll(v, 7, 0) for v in here]
        for k in range(nv):
            n = jnp.where(top, dn[k - 1] if k else 0.0, dn[k]) + jnp.where(
                bottom, up[k + 1] if k + 1 < nv else 0.0, up[k]
            )
            for other in (below, above):
                if other is not None:
                    n = n + other[k]
            emit(y * NZ + 8 * k, n)
        below, here = here, above


def rows8(base, r):
    return pl.ds(pl.multiple_of(base + r, 8), 8)


def local_pass(half, w, a2, prior, out):
    def plane(base, lo, hi):
        def emit(r, n):
            if lo:
                n = n + w[rows8(base, r - PLANE), :]
            if hi:
                n = n + w[rows8(base, r + PLANE), :]
            v = a2[rows8(base, r), :] * n
            out[rows8(base, r), :] = 0.5 * v if half else v - prior[rows8(base, r), :]

        yz_sums(w, base, emit)

    plane(0, False, True)
    lax.fori_loop(1, NX - 1, lambda i, c: (plane(pl.multiple_of(i * PLANE, PLANE), True, True), c)[1], 0)
    plane((NX - 1) * PLANE, True, False)


def ghost_pass(half, g, inner, inner_base, a2, prior, out):
    def emit(r, n):
        v = a2[rows8(0, r), :] * (n + inner[rows8(inner_base, r), :])
        out[rows8(0, r), :] = 0.5 * v if half else v - prior[rows8(0, r), :]

    yz_sums(g, 0, emit)


def ghost_add(half, g, a2, outer, out):
    def body(i):
        rows = pl.ds(pl.multiple_of(i * 64, 64), 64)
        r = a2[rows, :] * outer[rows, :]
        out[rows, :] = g[rows, :] + (0.5 * r if half else r)

    loop(PLANE // 64, body)


def spread(tile, emit):
    st = jnp.transpose(tile, (1, 0))
    for j in range(NY):
        emit(j, jnp.broadcast_to(st[:NZ, j : j + 1], (NZ, C)))


def fill_cross(d, depth, values, sv):
    base = cross_base(depth)
    for i in range(PLANE // 128):
        rows = pl.ds(pl.multiple_of(base + i * 128, 128), 128)
        d[pl.ds(i * 128, 128), :] = values(rows)
    if sv is not None:
        up = side(*CROSS)
        d[PLANE:, :] = jnp.zeros((SCALES, C), F32)
        d[PLANE:, :NZ] = sv[up * (NX - depth) + (1 - up) * (depth - 1)]


def first_kernel(feat, scales, d1, buf, sv, sems):
    up = side(*CROSS)
    two = [
        pltpu.make_async_copy(scales.at[up * (NX - 1)], sv, sems.at[0]),
        pltpu.make_async_copy(feat.at[pl.ds(cross_base(1), PLANE), :], buf, sems.at[1]),
    ]
    for c in two:
        c.start()
    two[0].wait()
    tile = sv[...]
    d1[PLANE:, :] = jnp.zeros((SCALES, C), F32)
    d1[PLANE:, :NZ] = tile
    two[1].wait()

    def emit(j, b):
        rows = pl.ds(j * NZ, NZ)
        d1[rows, :] = b * buf[rows, :]

    spread(tile, emit)


def start_kernel(feat, scales, fv, sb, d2, d3, *rest):
    sends, (sv, sems) = rest[:5], rest[5:]
    first = pltpu.make_async_copy(scales, sv, sems.at[NX])
    first.start()

    def copy(i):
        rows = pl.ds(i * PLANE, PLANE)
        return pltpu.make_async_copy(feat.at[rows, :], fv.at[rows, :], sems.at[i])

    for i in range(NX):
        copy(i).start()
    first.wait()
    for i in range(NX):

        def emit(j, b, i=i):
            sb[pl.ds(i * PLANE + j * NZ, NZ), :] = b

        spread(sv[i], emit)
    for i in range(NX):
        copy(i).wait()
    fill_cross(d2, 2, lambda rows: sb[rows, :] * fv[rows, :], sv)
    fill_cross(d3, 3, lambda rows: sb[rows, :] * fv[rows, :], None)
    for (axis, kind), send in zip(LOCALS, sends):
        at = face_slices(axis, kind)
        for group in batches(axis):
            got = [sb[at(i)[0], :] * fv[at(i)[0], :] for i in group]
            for i, v in zip(group, got):
                send[at(i)[1], :] = v


def aux_kernel(sb, fv, weights, w0, a2, w4, *faces):
    def body(i):
        rows = pl.ds(pl.multiple_of(i * 128, 128), 128)
        s = sb[rows, :]
        w0[rows, :] = s * fv[rows, :]
        a2[rows, :] = -2.0 * (s * s)

    loop(ROWS // 128, body, 1)
    for (axis, kind), face in zip(LOCALS, faces):
        emit_face(a2, axis, kind, face)
    for layer in range(2):
        w = weights[layer]
        hi = w.astype(jnp.bfloat16)
        lo = (w - hi.astype(F32)).astype(jnp.bfloat16)
        both = jnp.concatenate([hi, lo], axis=1)
        w4[layer, :C, :] = both
        w4[layer, C:, :] = both


def ghost_aux_kernel(d, a2g):
    def emit(j, b):
        a2g[pl.ds(j * NZ, NZ), :] = -2.0 * (b * b)

    spread(d[PLANE:, :], emit)


def local1_kernel(w0, a2, w1):
    local_pass(True, w0, a2, None, w1)


def local2_kernel(w1, a2, w0, d1, a2g1, w2, p1):
    local_pass(False, w1, a2, w0, w2)
    ghost_pass(True, d1, w0, cross_base(1), a2g1, None, p1)


def local3_kernel(w2, a2, w1, d1, d2, w1g1, a2g1, a2g2, w3, p2, q1):
    local_pass(False, w2, a2, w1, w3)
    ghost_pass(True, d2, d1, 0, a2g2, None, p2)
    ghost_pass(False, w1g1, w1, cross_base(1), a2g1, d1, q1)


def fix1_kernel(w_in, a2, z1, z0, d1, *rest):
    halos, w, sends = rest[:5], rest[5], rest[6:]
    fix_faces(True, w, a2, (z1, z0), halos, d1, sends)
    emit_ghost_lines((d1,), sends)


def fix2_kernel(w_in, a2, z1, z0, d2, p1, a2g1, *rest):
    halos, w, w1g1, sends = rest[:5], rest[5], rest[6], rest[7:]
    ghost_add(True, p1, a2g1, d2, w1g1)
    fix_lines(True, w1g1, a2g1, halos, 0)
    fix_faces(False, w, a2, (z1, z0), halos, w1g1, sends)
    emit_ghost_lines((w1g1, d2), sends)


def fix3(w, a2, zfaces, d3, p2, q1, a2g1, a2g2, halos, g2, g1, faces):
    ghost_add(True, p2, a2g2, d3, g2)
    fix_lines(True, g2, a2g2, halos, 1)
    ghost_add(False, q1, a2g1, g2, g1)
    fix_lines(False, g1, a2g1, halos, 0)
    fix_faces(False, w, a2, zfaces, halos, g1, (*faces, None))


def mixed(layer, ws, a2, thetas, w4, rows, scaled):
    t = None
    for k, w in enumerate(ws):
        term = thetas[layer, k : k + 1, :] * w[rows, :]
        t = term if t is None else t + term
    hi = t.astype(jnp.bfloat16)
    lo = (t - hi.astype(F32)).astype(jnp.bfloat16)
    both = jnp.dot(jnp.concatenate([hi, lo], axis=1), w4[layer], preferred_element_type=F32)
    q = -0.5 * a2[rows, :]
    r = lax.rsqrt(q)
    h = (both[:, :C] + both[:, C:]) * (0.5 * r)
    out = h + h * jnp.tanh(h)
    return (q * r) * out if scaled else out


def mix_planes(layer, ws, a2, thetas, w4, key, dst, scaled, at=0):
    base = side(*key) * ((NX - 1) * PLANE)
    for i in range(PLANE // 256):
        rows = pl.ds(pl.multiple_of(base + i * 256, 256), 256)
        dst[pl.ds(at + i * 256, 256), :] = mixed(layer, ws, a2, thetas, w4, rows, scaled)


def cross_mix_kernel(layer, w3_in, a2, z1, z0, d3, p2, q1, a2g1, a2g2, w0, w1, w2, thetas, w4, *rest):
    halos, w3, d1, faces, (g2, g1) = rest[:5], rest[5], rest[6], rest[7:11], rest[11:]
    fix3(w3, a2, (z1, z0), d3, p2, q1, a2g1, a2g2, halos, g2, g1, faces)
    mix_planes(layer, (w0, w1, w2, w3), a2, thetas, w4, CROSS, d1, True)


def mix_faces(layer, f, thetas, w4, outs, scaled):
    for (axis, _), (*ws, a2), out in zip(LOCALS, f, outs):
        for i in range(FACE[axis] // 256):
            rows = pl.ds(i * 256, 256)
            out[rows, :] = mixed(layer, ws, a2, thetas, w4, rows, scaled)


def face_mix_kernel(layer, a2, w0, w1, w2, w3, thetas, w4, *rest):
    f, sends = [rest[i :20:4] for i in range(4)], rest[20:]
    mix_faces(layer, f, thetas, w4, sends, True)
    mix_planes(layer, (w0, w1, w2, w3), a2, thetas, w4, LOCALS[-1], sends[-1], True)


def inner_mix_kernel(layer, scaled, w0, w1, w2, w3, a2, thetas, w4, out):
    def body(i):
        rows = pl.ds(pl.multiple_of(PLANE + i * 256, 256), 256)
        out[rows, :] = mixed(layer, (w0, w1, w2, w3), a2, thetas, w4, rows, scaled)

    loop((ROWS - 2 * PLANE) // 256, body, 4)


def put_faces(out, faces):
    for (axis, kind), face in zip(LOCALS, faces):
        at = face_slices(axis, kind)
        for group in batches(axis):
            got = [face[at(i)[1], :] for i in group]
            for i, v in zip(group, got):
                out[at(i)[0], :] = v


def merge_kernel(inner, d1, *rest):
    sends, out, d2, d3 = rest[:5], *rest[5:]
    put_faces(out, sends)
    base = cross_base(1)
    for i in range(PLANE // 128):
        out[pl.ds(pl.multiple_of(base + i * 128, 128), 128), :] = d1[pl.ds(i * 128, 128), :]
    copy_plane(out, cross_base(2), d2)
    copy_plane(out, cross_base(3), d3)


def last_kernel(layer, w3_in, a2, z1, z0, d3, p2, q1, a2g1, a2g2, w0, w1, w2, thetas, w4, inner, *rest):
    halos, known = rest[:5], rest[5:21]
    (w3, hidden, out), (g2, g1), faces, done, sems = rest[21:24], rest[24:26], rest[26:30], rest[30:34], rest[34]
    fix3(w3, a2, (z1, z0), d3, p2, q1, a2g1, a2g2, halos, g2, g1, faces)

    def copy(i):
        rows = pl.ds(pl.multiple_of(i * PLANE, PLANE), PLANE)
        return pltpu.make_async_copy(hidden.at[rows, :], out.at[rows, :], sems.at[i])

    f = [(*known[i:12:4], faces[i], known[12 + i]) for i in range(4)]
    mix_faces(layer, f, thetas, w4, done, False)
    put_faces(hidden, done)
    for i in range(1, NX - 1):
        copy(i).start()
    for i in range(2 * PLANE // 256):
        plane, part = divmod(i, PLANE // 256)
        rows = pl.ds(plane * (NX - 1) * PLANE + part * 256, 256)
        hidden[rows, :] = mixed(layer, (w0, w1, w2, w3), a2, thetas, w4, rows, False)
    copy(0).start()
    copy(NX - 1).start()
    loop(NX, lambda i: copy(i).wait(), 1)


def call(kernel, out_shape, args, in_hbm=(), out_hbm=(), scratch=(), aliases=None, mib=1):
    return pl.pallas_call(
        kernel,
        out_shape=out_shape,
        in_specs=[HBM if i in in_hbm else VM for i in range(len(args))],
        out_specs=[HBM if i in out_hbm else VM for i in range(len(out_shape))],
        scratch_shapes=list(scratch),
        input_output_aliases=aliases or {},
        compiler_params=pltpu.CompilerParams(vmem_limit_bytes=mib * MIB),
    )(*args)


def per_device(features, scales, thetas, weights):
    shape = features.shape
    feat = pltpu.with_memory_space_constraint(features.reshape(ROWS, C), pltpu.HBM)
    block, plane = arr(ROWS), arr(PLANE)
    scales = pltpu.with_memory_space_constraint(scales, pltpu.HBM)
    ghosts = [pltpu.VMEM((PLANE, C), F32)] * 2
    (s1,) = call(
        first_kernel,
        [arr(PLANE + SCALES)],
        (feat, scales),
        in_hbm=(0, 1),
        scratch=[pltpu.VMEM((PLANE, C), F32), pltpu.VMEM((NY, NZ), F32), pltpu.SemaphoreType.DMA((2,))],
    )
    fv, sb, s2, s3, *sends = call(
        start_kernel,
        [block, block, arr(PLANE + SCALES), plane] + locals_out(0),
        (feat, scales),
        in_hbm=(0, 1),
        scratch=[pltpu.VMEM(scales.shape, F32), pltpu.SemaphoreType.DMA((NX + 1,))],
    )
    for layer in range(2):
        last = layer == 1
        if last:
            w0, s2, s3 = call(merge_kernel, [block, plane, plane], (inner, s1, *sends), aliases={0: 0})
        known = [sends[:4]]
        (d1,), halos, (d2,) = exchange(sends, cross=s1, late=s2)
        if not last:
            w4 = jax.ShapeDtypeStruct((2, 2 * C, 2 * C), jnp.bfloat16)
            w0, a2, w4, *af = call(aux_kernel, [block, block, w4] + locals_out(0)[:4], (sb, fv, weights))
            main = (a2, af[2], af[3])
        (w1,) = call(local1_kernel, [block], (w0, a2))
        w1, *sends = call(fix1_kernel, [block] + locals_out(1), (w1, *main, d1, *halos), aliases={0: 0})
        known.append(sends[:4])
        _, halos, (d3,) = exchange(sends, late=s3)
        if not last:
            (a2g1,) = call(ghost_aux_kernel, [plane], (d1,))
        w2, p1 = call(local2_kernel, [block, plane], (w1, a2, w0, d1, a2g1))
        w2, w1g1, *sends = call(
            fix2_kernel, [block, plane] + locals_out(2), (w2, *main, d2, p1, a2g1, *halos), aliases={0: 0}
        )
        known.append(sends[:4])
        _, halos, _ = exchange(sends)
        if not last:
            (a2g2,) = call(ghost_aux_kernel, [plane], (d2,))
        w3, p2, q1 = call(local3_kernel, [block, plane, plane], (w2, a2, w1, d1, d2, w1g1, a2g1, a2g2))
        (inner,) = call(functools.partial(inner_mix_kernel, layer, not last), [block], (w0, w1, w2, w3, a2, thetas, w4))
        tail = (w3, *main, d3, p2, q1, a2g1, a2g2, w0, w1, w2, thetas, w4)
        if not last:
            w3, s1, *faces = call(
                functools.partial(cross_mix_kernel, layer),
                [block, plane] + locals_out(0)[:4],
                (*tail, *halos),
                scratch=ghosts,
                aliases={0: 0},
            )
            sends = call(
                functools.partial(face_mix_kernel, layer),
                locals_out(0),
                (a2, w0, w1, w2, w3, thetas, w4, *sum(map(list, known), []), *faces, *af),
            )
        else:
            small = [pltpu.VMEM(a.shape, F32) for a in locals_out(0)[:4]]
            n = len(tail)
            _, _, out = call(
                functools.partial(last_kernel, layer),
                [block, block, block],
                (*tail, inner, *halos, *sum(map(list, known), []), *af),
                out_hbm=(2,),
                scratch=ghosts + small + small + [pltpu.SemaphoreType.DMA((NX,))],
                mib=3,
                aliases={0: 0, n: 1},
            )
    return out.reshape(shape)


def solution(mesh):
    return jax.shard_map(
        per_device,
        mesh=mesh,
        in_specs=(P(*AXES, None), P(*AXES), P(), P()),
        out_specs=P(*AXES, None),
        check_vma=False,
    )
```

```python
import functools

import jax
import jax.numpy as jnp
from jax import lax
from jax.experimental import pallas as pl
from jax.experimental.pallas import tpu as pltpu
from jax.sharding import PartitionSpec as P


AXES = ("gx", "gy", "gz")
NX, NY, NZ, C = 16, 16, 32, 128
PLANE = NY * NZ
ROWS = NX * PLANE
FACE = {"gx": PLANE, "gy": NX * NZ, "gz": NX * NY}
LINE = {"gy": NZ, "gz": NY}
CROSS = ("gx", 1)
LOCALS = (("gy", 0), ("gy", 1), ("gz", 1), ("gz", 0), ("gx", 0))
EARLY = (1, 9)
SCALES = 16

F32 = jnp.float32
VM = pl.BlockSpec(memory_space=pltpu.VMEM)
HBM = pl.BlockSpec(memory_space=pltpu.HBM)
MIB = 1024 * 1024


def arr(rows, cols=C, dtype=F32):
    return jax.ShapeDtypeStruct((rows, cols), dtype)


def locals_out(lines):
    return [arr(FACE[a] + lines * LINE.get(a, 0)) for a, _ in LOCALS]


def swap(x, axis, kind):
    n = lax.axis_size(axis)
    pairs = []
    for i in range(kind, n + kind, 2):
        a, b = i % n, (i + 1) % n
        pairs += [(a, b), (b, a)]
    return lax.ppermute(x, axis, pairs)


def exchange(sends, cross=None, late=None):
    first = [] if cross is None else [swap(cross, *CROSS)]
    got = [swap(s, a, k) for s, (a, k) in zip(sends, LOCALS)]
    last = [] if late is None else [swap(late, *CROSS)]
    return first, got, last


def side(axis, kind):
    odd = lax.rem(lax.axis_index(axis), 2)
    return odd if kind else 1 - odd


def face_slices(axis, kind):
    up = side(axis, kind)
    if axis == "gx":
        base = up * ((NX - 1) * PLANE)
        return lambda i: (pl.ds(pl.multiple_of(base + i * NZ, NZ), NZ), pl.ds(pl.multiple_of(i * NZ, NZ), NZ))
    if axis == "gy":
        base = up * ((NY - 1) * NZ)
        return lambda i: (pl.ds(pl.multiple_of(base + i * PLANE, NZ), NZ), pl.ds(pl.multiple_of(i * NZ, NZ), NZ))
    base = up * (NZ - 1)
    return lambda i: (pl.ds(base + i * PLANE, NY, stride=NZ), pl.ds(pl.multiple_of(i * NY, NY), NY))


def plane_line(axis, kind):
    up = side(axis, kind)
    if axis == "gy":
        return pl.ds(pl.multiple_of(up * ((NY - 1) * NZ), NZ), NZ)
    return pl.ds(up * (NZ - 1), NY, stride=NZ)


def line_rows(axis, i):
    return pl.ds(FACE[axis] + i * LINE[axis], LINE[axis])


def cross_base(depth):
    up = side(*CROSS)
    return pl.multiple_of(up * ((NX - depth) * PLANE) + (1 - up) * ((depth - 1) * PLANE), PLANE)


def loop(n, body, unroll=4):
    def step(i, c):
        body(i)
        return c

    lax.fori_loop(0, n, step, 0, unroll=unroll)


def copy_plane(src, base, dst):
    for i in range(PLANE // 128):
        rows = pl.ds(i * 128, 128)
        dst[rows, :] = src[pl.ds(pl.multiple_of(base + i * 128, 128), 128), :]


def batches(axis):
    size = 8 if axis == "gz" else 4
    return [range(g, g + size) for g in range(0, NX, size)]


def emit_face(w, axis, kind, send):
    at = face_slices(axis, kind)
    for group in batches(axis):
        got = [w[at(i)[0], :] for i in group]
        for i, v in zip(group, got):
            send[at(i)[1], :] = v


def fix_faces(half, w, a2, zfaces, halos, cross, sends):
    local = list(zip(LOCALS, halos, sends))
    plain = [(CROSS, cross)] + [(k, h) for k, h, _ in local if k[0] == "gx"] + [(k, h) for k, h, _ in local if k[0] == "gy"]
    for key, halo in plain:
        at = face_slices(*key)
        for group in batches(key[0]):
            got = []
            for i in group:
                dst, src = at(i)
                r = a2[dst, :] * halo[src, :]
                got.append(w[dst, :] + (0.5 * r if half else r))
            for i, v in zip(group, got):
                w[at(i)[0], :] = v
    for ((key, halo, send), face) in zip([t for t in local if t[0][0] == "gz"], zfaces):
        at = face_slices(*key)
        for group in batches("gz"):
            got = []
            for i in group:
                dst, src = at(i)
                r = face[src, :] * halo[src, :]
                got.append(w[dst, :] + (0.5 * r if half else r))
            for i, v in zip(group, got):
                w[at(i)[0], :] = v
                send[at(i)[1], :] = v
    for (axis, kind), _, send in local:
        if axis != "gz" and send is not None:
            emit_face(w, axis, kind, send)


def emit_ghost_lines(ghosts, sends):
    for (axis, kind), send in zip(LOCALS, sends):
        if axis != "gx":
            for i, g in enumerate(ghosts):
                send[line_rows(axis, i), :] = g[plane_line(axis, kind), :]


def fix_lines(half, g, a2, halos, i):
    for (axis, kind), halo in zip(LOCALS, halos):
        if axis == "gx":
            continue
        at = plane_line(axis, kind)
        r = a2[at, :] * halo[line_rows(axis, i), :]
        g[at, :] = g[at, :] + (0.5 * r if half else r)


def yz_sums(w, base, emit):
    sub = lax.broadcasted_iota(jnp.int32, (8, C), 0)
    top, bottom = sub == 0, sub == 7
    nv = NZ // 8

    def at(y):
        return [w[pl.ds(pl.multiple_of(base + y * NZ + 8 * k, 8), 8), :] for k in range(nv)]

    below, here = None, at(0)
    for y in range(NY):
        above = at(y + 1) if y + 1 < NY else None
        dn = [pltpu.roll(v, 1, 0) for v in here]
        up = [pltpu.roll(v, 7, 0) for v in here]
        for k in range(nv):
            n = jnp.where(top, dn[k - 1] if k else 0.0, dn[k]) + jnp.where(
                bottom, up[k + 1] if k + 1 < nv else 0.0, up[k]
            )
            for other in (below, above):
                if other is not None:
                    n = n + other[k]
            emit(y * NZ + 8 * k, n)
        below, here = here, above


def rows8(base, r):
    return pl.ds(pl.multiple_of(base + r, 8), 8)


def local_pass(half, w, a2, prior, out):
    def plane(base, lo, hi):
        def emit(r, n):
            if lo:
                n = n + w[rows8(base, r - PLANE), :]
            if hi:
                n = n + w[rows8(base, r + PLANE), :]
            v = a2[rows8(base, r), :] * n
            out[rows8(base, r), :] = 0.5 * v if half else v - prior[rows8(base, r), :]

        yz_sums(w, base, emit)

    plane(0, False, True)
    lax.fori_loop(1, NX - 1, lambda i, c: (plane(pl.multiple_of(i * PLANE, PLANE), True, True), c)[1], 0)
    plane((NX - 1) * PLANE, True, False)


def ghost_pass(half, g, inner, inner_base, a2, prior, out):
    def emit(r, n):
        v = a2[rows8(0, r), :] * (n + inner[rows8(inner_base, r), :])
        out[rows8(0, r), :] = 0.5 * v if half else v - prior[rows8(0, r), :]

    yz_sums(g, 0, emit)


def ghost_add(half, g, a2, outer, out):
    def body(i):
        rows = pl.ds(pl.multiple_of(i * 64, 64), 64)
        r = a2[rows, :] * outer[rows, :]
        out[rows, :] = g[rows, :] + (0.5 * r if half else r)

    loop(PLANE // 64, body)


def spread(tile, emit):
    st = jnp.transpose(tile, (1, 0))
    for j in range(NY):
        emit(j, jnp.broadcast_to(st[:NZ, j : j + 1], (NZ, C)))


def first_kernel(feat, scales, d1, buf, sv, sems):
    up = side(*CROSS)
    two = [
        pltpu.make_async_copy(scales.at[up * (NX - 1)], sv, sems.at[0]),
        pltpu.make_async_copy(feat.at[pl.ds(cross_base(1), PLANE), :], buf, sems.at[1]),
    ]
    for c in two:
        c.start()
    two[0].wait()
    tile = sv[...]
    d1[PLANE:, :] = jnp.zeros((SCALES, C), F32)
    d1[PLANE:, :NZ] = tile
    two[1].wait()

    def emit(j, b):
        rows = pl.ds(j * NZ, NZ)
        d1[rows, :] = b * buf[rows, :]

    spread(tile, emit)


def start_kernel(fv, sv, d2, d3, *sends):
    up = side(*CROSS)
    for depth, d in ((2, d2), (3, d3), (0, sends[-1])):
        plane = up * (NX - depth) + (1 - up) * (depth - 1) if depth else (1 - up) * (NX - 1)
        base = pl.multiple_of(plane * PLANE, PLANE)
        tile = sv[plane]

        def emit(j, b, base=base, d=d):
            d[pl.ds(j * NZ, NZ), :] = b * fv[pl.ds(pl.multiple_of(base + j * NZ, NZ), NZ), :]

        spread(tile, emit)
        if depth == 2:
            d[PLANE:, :] = jnp.zeros((SCALES, C), F32)
            d[PLANE:, :NZ] = tile
    for x in range(NX):
        tile = sv[x]
        st = jnp.transpose(tile, (1, 0))
        ends = {
            "gy": [
                jnp.broadcast_to(st[:, y : y + 1], (NZ, C)) * fv[pl.ds(x * PLANE + y * NZ, NZ), :] for y in (0, NY - 1)
            ],
            "gz": [
                jnp.broadcast_to(tile[:, z : z + 1], (NY, C)) * fv[pl.ds(x * PLANE + z, NY, stride=NZ), :]
                for z in (0, NZ - 1)
            ],
        }
        for (axis, kind), send in zip(LOCALS[:-1], sends):
            low, high = ends[axis]
            send[pl.ds(x * LINE[axis], LINE[axis]), :] = jnp.where(side(axis, kind) == 1, high, low)


def aux_kernel(sv, fv, weights, w0, a2, w4, *faces):
    for x in range(NX):

        def emit(j, b, x=x):
            rows = pl.ds(x * PLANE + j * NZ, NZ)
            w0[rows, :] = b * fv[rows, :]
            a2[rows, :] = -2.0 * (b * b)

        spread(sv[x], emit)
    for (axis, kind), face in zip(LOCALS, faces):
        emit_face(a2, axis, kind, face)
    for layer in range(2):
        w = weights[layer]
        hi = w.astype(jnp.bfloat16)
        lo = (w - hi.astype(F32)).astype(jnp.bfloat16)
        both = jnp.concatenate([hi, lo], axis=1)
        w4[layer, :C, :] = both
        w4[layer, C:, :] = both


def ghost_aux_kernel(d, a2g):
    def emit(j, b):
        a2g[pl.ds(j * NZ, NZ), :] = -2.0 * (b * b)

    spread(d[PLANE:, :], emit)


def local1_kernel(w0, a2, w1):
    local_pass(True, w0, a2, None, w1)


def local2_kernel(w1, a2, w0, d1, a2g1, w2, p1):
    local_pass(False, w1, a2, w0, w2)
    ghost_pass(True, d1, w0, cross_base(1), a2g1, None, p1)


def local3_kernel(w2, a2, w1, d1, d2, w1g1, a2g1, a2g2, w3, p2, q1):
    local_pass(False, w2, a2, w1, w3)
    ghost_pass(True, d2, d1, 0, a2g2, None, p2)
    ghost_pass(False, w1g1, w1, cross_base(1), a2g1, d1, q1)


def fix1_kernel(w_in, a2, z1, z0, d1, *rest):
    halos, w, sends = rest[:5], rest[5], rest[6:]
    fix_faces(True, w, a2, (z1, z0), halos, d1, sends)
    emit_ghost_lines((d1,), sends)


def fix2_kernel(w_in, a2, z1, z0, d2, p1, a2g1, *rest):
    halos, w, w1g1, sends = rest[:5], rest[5], rest[6], rest[7:]
    ghost_add(True, p1, a2g1, d2, w1g1)
    fix_lines(True, w1g1, a2g1, halos, 0)
    fix_faces(False, w, a2, (z1, z0), halos, w1g1, sends)
    emit_ghost_lines((w1g1, d2), sends)


def fix3(w, a2, zfaces, d3, p2, q1, a2g1, a2g2, halos, g2, g1, faces):
    ghost_add(True, p2, a2g2, d3, g2)
    fix_lines(True, g2, a2g2, halos, 1)
    ghost_add(False, q1, a2g1, g2, g1)
    fix_lines(False, g1, a2g1, halos, 0)
    fix_faces(False, w, a2, zfaces, halos, g1, (*faces, None))


def mixed(layer, ws, a2, thetas, w4, rows, scaled):
    t = None
    for k, w in enumerate(ws):
        term = thetas[layer, k : k + 1, :] * w[rows, :]
        t = term if t is None else t + term
    hi = t.astype(jnp.bfloat16)
    lo = (t - hi.astype(F32)).astype(jnp.bfloat16)
    both = jnp.dot(jnp.concatenate([hi, lo], axis=1), w4[layer], preferred_element_type=F32)
    q = -0.5 * a2[rows, :]
    r = lax.rsqrt(q)
    h = (both[:, :C] + both[:, C:]) * (0.5 * r)
    out = h + h * jnp.tanh(h)
    return (q * r) * out if scaled else out


def mix_planes(layer, ws, a2, thetas, w4, key, dst, scaled, at=0):
    base = side(*key) * ((NX - 1) * PLANE)
    for i in range(PLANE // 256):
        rows = pl.ds(pl.multiple_of(base + i * 256, 256), 256)
        dst[pl.ds(at + i * 256, 256), :] = mixed(layer, ws, a2, thetas, w4, rows, scaled)


def cross_mix_kernel(layer, w3_in, a2, z1, z0, d3, p2, q1, a2g1, a2g2, w0, w1, w2, thetas, w4, *rest):
    halos, w3, d1, faces, (g2, g1) = rest[:5], rest[5], rest[6], rest[7:11], rest[11:]
    fix3(w3, a2, (z1, z0), d3, p2, q1, a2g1, a2g2, halos, g2, g1, faces)
    mix_planes(layer, (w0, w1, w2, w3), a2, thetas, w4, CROSS, d1, True)


def mix_faces(layer, f, thetas, w4, outs, scaled, planes=(0, NX)):
    for (axis, _), (*ws, a2), out in zip(LOCALS, f, outs):
        start, stop = planes[0] * LINE[axis], planes[1] * LINE[axis]
        size = min(256, stop - start)
        for at in range(start, stop, size):
            rows = pl.ds(at, size)
            out[rows, :] = mixed(layer, ws, a2, thetas, w4, rows, scaled)


def face_mix_kernel(layer, a2, w0, w1, w2, w3, thetas, w4, *rest):
    f, sends = [rest[i :20:4] for i in range(4)], rest[20:]
    mix_faces(layer, f, thetas, w4, sends, True)
    mix_planes(layer, (w0, w1, w2, w3), a2, thetas, w4, LOCALS[-1], sends[-1], True)


def mix_range(layer, scaled, ws, a2, thetas, w4, out, planes, then=None):
    for x in range(*planes):
        for part in range(PLANE // 256):
            rows = pl.ds(x * PLANE + part * 256, 256)
            out[rows, :] = mixed(layer, ws, a2, thetas, w4, rows, scaled)
        if then is not None:
            then(x)


def inner_mix_kernel(layer, scaled, w0, w1, w2, w3, a2, thetas, w4, out):
    mix_range(layer, scaled, (w0, w1, w2, w3), a2, thetas, w4, out, EARLY)


def put_faces(out, faces, planes):
    for (axis, kind), face in zip(LOCALS, faces):
        at = face_slices(axis, kind)
        for g in range(*planes, 4):
            group = range(g, min(g + 4, planes[1]))
            got = [face[at(i)[1], :] for i in group]
            for i, v in zip(group, got):
                out[at(i)[0], :] = v


def merge_kernel(layer, inner, d1, w0, w1, w2, w3, a2, thetas, w4, *rest):
    sends, out, d2, d3 = rest[:5], *rest[5:]
    put_faces(out, sends[:-1], EARLY)
    for key, face in ((CROSS, d1), (LOCALS[-1], sends[-1])):
        base = side(*key) * ((NX - 1) * PLANE)
        for i in range(PLANE // 128):
            out[pl.ds(pl.multiple_of(base + i * 128, 128), 128), :] = face[pl.ds(i * 128, 128), :]
    mix_range(layer, True, (w0, w1, w2, w3), a2, thetas, w4, out, (EARLY[1], NX - 1))
    copy_plane(out, cross_base(2), d2)
    copy_plane(out, cross_base(3), d3)


def last_kernel(layer, w3_in, a2, z1, z0, d3, p2, q1, a2g1, a2g2, w0, w1, w2, thetas, w4, inner, *rest):
    halos, known = rest[:5], rest[5:21]
    (w3, hidden, out), (g2, g1), faces, done, sems = rest[21:24], rest[24:26], rest[26:30], rest[30:34], rest[34]
    fix3(w3, a2, (z1, z0), d3, p2, q1, a2g1, a2g2, halos, g2, g1, faces)

    def copy(i):
        rows = pl.ds(i * PLANE, PLANE)
        return pltpu.make_async_copy(hidden.at[rows, :], out.at[rows, :], sems.at[i])

    f = [(*known[i:12:4], faces[i], known[12 + i]) for i in range(4)]
    mix_faces(layer, f, thetas, w4, done, False, EARLY)
    put_faces(hidden, done, EARLY)
    for i in range(*EARLY):
        copy(i).start()
    ws = (w0, w1, w2, w3)
    for planes in ((0, EARLY[0]), (EARLY[1], NX)):
        mix_range(layer, False, ws, a2, thetas, w4, hidden, planes, lambda x: copy(x).start())
    for i in range(NX):
        copy(i).wait()


def call(kernel, out_shape, args, in_hbm=(), out_hbm=(), scratch=(), aliases=None, mib=1):
    return pl.pallas_call(
        kernel,
        out_shape=out_shape,
        in_specs=[HBM if i in in_hbm else VM for i in range(len(args))],
        out_specs=[HBM if i in out_hbm else VM for i in range(len(out_shape))],
        scratch_shapes=list(scratch),
        input_output_aliases=aliases or {},
        compiler_params=pltpu.CompilerParams(vmem_limit_bytes=mib * MIB),
    )(*args)


def per_device(features, scales, thetas, weights):
    shape = features.shape
    fv, sv = features.reshape(ROWS, C), scales
    feat = pltpu.with_memory_space_constraint(fv, pltpu.HBM)
    block, plane = arr(ROWS), arr(PLANE)
    scales = pltpu.with_memory_space_constraint(scales, pltpu.HBM)
    ghosts = [pltpu.VMEM((PLANE, C), F32)] * 2
    (s1,) = call(
        first_kernel,
        [arr(PLANE + SCALES)],
        (feat, scales),
        in_hbm=(0, 1),
        scratch=[pltpu.VMEM((PLANE, C), F32), pltpu.VMEM((NY, NZ), F32), pltpu.SemaphoreType.DMA((2,))],
    )
    s2, s3, *sends = call(start_kernel, [arr(PLANE + SCALES), plane] + locals_out(0), (fv, sv))
    for layer in range(2):
        last = layer == 1
        if last:
            w0, s2, s3 = call(
                functools.partial(merge_kernel, 0),
                [block, plane, plane],
                (inner, s1, w0, w1, w2, w3, a2, thetas, w4, *sends),
                aliases={0: 0},
            )
        known = [sends[:4]]
        (d1,), halos, (d2,) = exchange(sends, cross=s1, late=s2)
        if not last:
            w4 = jax.ShapeDtypeStruct((2, 2 * C, 2 * C), jnp.bfloat16)
            w0, a2, w4, *af = call(aux_kernel, [block, block, w4] + locals_out(0)[:4], (sv, fv, weights))
            main = (a2, af[2], af[3])
        (w1,) = call(local1_kernel, [block], (w0, a2))
        w1, *sends = call(fix1_kernel, [block] + locals_out(1), (w1, *main, d1, *halos), aliases={0: 0})
        known.append(sends[:4])
        _, halos, (d3,) = exchange(sends, late=s3)
        if not last:
            (a2g1,) = call(ghost_aux_kernel, [plane], (d1,))
        w2, p1 = call(local2_kernel, [block, plane], (w1, a2, w0, d1, a2g1))
        w2, w1g1, *sends = call(
            fix2_kernel, [block, plane] + locals_out(2), (w2, *main, d2, p1, a2g1, *halos), aliases={0: 0}
        )
        known.append(sends[:4])
        _, halos, _ = exchange(sends)
        if not last:
            (a2g2,) = call(ghost_aux_kernel, [plane], (d2,))
        w3, p2, q1 = call(local3_kernel, [block, plane, plane], (w2, a2, w1, d1, d2, w1g1, a2g1, a2g2))
        (inner,) = call(functools.partial(inner_mix_kernel, layer, not last), [block], (w0, w1, w2, w3, a2, thetas, w4))
        tail = (w3, *main, d3, p2, q1, a2g1, a2g2, w0, w1, w2, thetas, w4)
        if not last:
            w3, s1, *faces = call(
                functools.partial(cross_mix_kernel, layer),
                [block, plane] + locals_out(0)[:4],
                (*tail, *halos),
                scratch=ghosts,
                aliases={0: 0},
            )
            sends = call(
                functools.partial(face_mix_kernel, layer),
                locals_out(0),
                (a2, w0, w1, w2, w3, thetas, w4, *sum(map(list, known), []), *faces, *af),
            )
        else:
            small = [pltpu.VMEM(a.shape, F32) for a in locals_out(0)[:4]]
            n = len(tail)
            _, _, out = call(
                functools.partial(last_kernel, layer),
                [block, block, block],
                (*tail, inner, *halos, *sum(map(list, known), []), *af),
                out_hbm=(2,),
                scratch=ghosts + small + small + [pltpu.SemaphoreType.DMA((NX,))],
                mib=3,
                aliases={0: 0, n: 1},
            )
    return out.reshape(shape)


def solution(mesh):
    return jax.shard_map(
        per_device,
        mesh=mesh,
        in_specs=(P(*AXES, None), P(*AXES), P(), P()),
        out_specs=P(*AXES, None),
        check_vma=False,
    )
```

```python
import functools

import jax
import jax.numpy as jnp
from jax import lax
from jax.experimental import pallas as pl
from jax.experimental.pallas import tpu as pltpu
from jax.sharding import PartitionSpec as P


AXES = ("gx", "gy", "gz")
NX, NY, NZ, C = 16, 16, 32, 128
PLANE = NY * NZ
ROWS = NX * PLANE
FACE = {"gx": PLANE, "gy": NX * NZ, "gz": NX * NY}
LINE = {"gy": NZ, "gz": NY}
CROSS = ("gx", 1)
LOCALS = (("gy", 0), ("gy", 1), ("gz", 1), ("gz", 0), ("gx", 0))
EARLY = (1, 9)
SCALES = 16

F32 = jnp.float32
VM = pl.BlockSpec(memory_space=pltpu.VMEM)
HBM = pl.BlockSpec(memory_space=pltpu.HBM)
MIB = 1024 * 1024


def arr(rows, cols=C, dtype=F32):
    return jax.ShapeDtypeStruct((rows, cols), dtype)


def locals_out(lines):
    return [arr(FACE[a] + lines * LINE.get(a, 0)) for a, _ in LOCALS]


def swap(x, axis, kind):
    n = lax.axis_size(axis)
    pairs = []
    for i in range(kind, n + kind, 2):
        a, b = i % n, (i + 1) % n
        pairs += [(a, b), (b, a)]
    return lax.ppermute(x, axis, pairs)


def exchange(sends, cross=None, late=None):
    first = [] if cross is None else [swap(cross, *CROSS)]
    got = [swap(s, a, k) for s, (a, k) in zip(sends, LOCALS)]
    last = [] if late is None else [swap(late, *CROSS)]
    return first, got, last


def side(axis, kind):
    odd = lax.rem(lax.axis_index(axis), 2)
    return odd if kind else 1 - odd


def face_slices(axis, kind):
    up = side(axis, kind)
    if axis == "gx":
        base = up * ((NX - 1) * PLANE)
        return lambda i: (pl.ds(pl.multiple_of(base + i * NZ, NZ), NZ), pl.ds(pl.multiple_of(i * NZ, NZ), NZ))
    if axis == "gy":
        base = up * ((NY - 1) * NZ)
        return lambda i: (pl.ds(pl.multiple_of(base + i * PLANE, NZ), NZ), pl.ds(pl.multiple_of(i * NZ, NZ), NZ))
    base = up * (NZ - 1)
    return lambda i: (pl.ds(base + i * PLANE, NY, stride=NZ), pl.ds(pl.multiple_of(i * NY, NY), NY))


def plane_line(axis, kind):
    up = side(axis, kind)
    if axis == "gy":
        return pl.ds(pl.multiple_of(up * ((NY - 1) * NZ), NZ), NZ)
    return pl.ds(up * (NZ - 1), NY, stride=NZ)


def line_rows(axis, i):
    return pl.ds(FACE[axis] + i * LINE[axis], LINE[axis])


def cross_base(depth):
    up = side(*CROSS)
    return pl.multiple_of(up * ((NX - depth) * PLANE) + (1 - up) * ((depth - 1) * PLANE), PLANE)


def copy_plane(src, base, dst):
    for i in range(PLANE // 128):
        rows = pl.ds(i * 128, 128)
        dst[rows, :] = src[pl.ds(pl.multiple_of(base + i * 128, 128), 128), :]


def batches(axis):
    size = 8 if axis == "gz" else 4
    return [range(g, g + size) for g in range(0, NX, size)]


def emit_face(w, axis, kind, send):
    at = face_slices(axis, kind)
    for group in batches(axis):
        got = [w[at(i)[0], :] for i in group]
        for i, v in zip(group, got):
            send[at(i)[1], :] = v


def fix_faces(half, w, a2, zfaces, halos, cross, sends):
    local = list(zip(LOCALS, halos, sends))
    plain = [(CROSS, cross)] + [(k, h) for k, h, _ in local if k[0] == "gx"] + [(k, h) for k, h, _ in local if k[0] == "gy"]
    for key, halo in plain:
        at = face_slices(*key)
        for group in batches(key[0]):
            got = []
            for i in group:
                dst, src = at(i)
                r = a2[dst, :] * halo[src, :]
                got.append(w[dst, :] + (0.5 * r if half else r))
            for i, v in zip(group, got):
                w[at(i)[0], :] = v
    for ((key, halo, send), face) in zip([t for t in local if t[0][0] == "gz"], zfaces):
        at = face_slices(*key)
        for group in batches("gz"):
            got = []
            for i in group:
                dst, src = at(i)
                r = face[src, :] * halo[src, :]
                got.append(w[dst, :] + (0.5 * r if half else r))
            for i, v in zip(group, got):
                w[at(i)[0], :] = v
                send[at(i)[1], :] = v
    for (axis, kind), _, send in local:
        if axis != "gz" and send is not None:
            emit_face(w, axis, kind, send)


def emit_ghost_lines(ghosts, sends):
    for (axis, kind), send in zip(LOCALS, sends):
        if axis != "gx":
            for i, g in enumerate(ghosts):
                send[line_rows(axis, i), :] = g[plane_line(axis, kind), :]


def fix_lines(half, g, a2, halos, i):
    for (axis, kind), halo in zip(LOCALS, halos):
        if axis == "gx":
            continue
        at = plane_line(axis, kind)
        r = a2[at, :] * halo[line_rows(axis, i), :]
        g[at, :] = g[at, :] + (0.5 * r if half else r)


def yz_sums(w, base, emit):
    sub = lax.broadcasted_iota(jnp.int32, (8, C), 0)
    top, bottom = sub == 0, sub == 7
    nv = NZ // 8

    def at(y):
        return [w[pl.ds(pl.multiple_of(base + y * NZ + 8 * k, 8), 8), :] for k in range(nv)]

    below, here = None, at(0)
    for y in range(NY):
        above = at(y + 1) if y + 1 < NY else None
        dn = [pltpu.roll(v, 1, 0) for v in here]
        up = [pltpu.roll(v, 7, 0) for v in here]
        for k in range(nv):
            n = jnp.where(top, dn[k - 1] if k else 0.0, dn[k]) + jnp.where(
                bottom, up[k + 1] if k + 1 < nv else 0.0, up[k]
            )
            for other in (below, above):
                if other is not None:
                    n = n + other[k]
            emit(y * NZ + 8 * k, n)
        below, here = here, above


def rows8(base, r):
    return pl.ds(pl.multiple_of(base + r, 8), 8)


def local_pass(half, w, a2, prior, out):
    def plane(base, lo, hi):
        def emit(r, n):
            if lo:
                n = n + w[rows8(base, r - PLANE), :]
            if hi:
                n = n + w[rows8(base, r + PLANE), :]
            v = a2[rows8(base, r), :] * n
            out[rows8(base, r), :] = 0.5 * v if half else v - prior[rows8(base, r), :]

        yz_sums(w, base, emit)

    plane(0, False, True)
    lax.fori_loop(1, NX - 1, lambda i, c: (plane(pl.multiple_of(i * PLANE, PLANE), True, True), c)[1], 0)
    plane((NX - 1) * PLANE, True, False)


def ghost_pass(half, g, inner, inner_base, outer, a2, prior, out):
    def emit(r, n):
        v = a2[rows8(0, r), :] * (n + inner[rows8(inner_base, r), :] + outer[rows8(0, r), :])
        out[rows8(0, r), :] = 0.5 * v if half else v - prior[rows8(0, r), :]

    yz_sums(g, 0, emit)


def spread(tile, emit):
    st = jnp.transpose(tile, (1, 0))
    for j in range(NY):
        emit(j, jnp.broadcast_to(st[:NZ, j : j + 1], (NZ, C)))


def first_kernel(feat, scales, d1, buf, sv, sems):
    up = side(*CROSS)
    two = [
        pltpu.make_async_copy(scales.at[up * (NX - 1)], sv, sems.at[0]),
        pltpu.make_async_copy(feat.at[pl.ds(cross_base(1), PLANE), :], buf, sems.at[1]),
    ]
    for c in two:
        c.start()
    two[0].wait()
    tile = sv[...]
    d1[PLANE:, :] = jnp.zeros((SCALES, C), F32)
    d1[PLANE:, :NZ] = tile
    two[1].wait()

    def emit(j, b):
        rows = pl.ds(j * NZ, NZ)
        d1[rows, :] = b * buf[rows, :]

    spread(tile, emit)


def start_kernel(fv, sv, d2, d3, *sends):
    up = side(*CROSS)
    for depth, d in ((2, d2), (3, d3), (0, sends[-1])):
        plane = up * (NX - depth) + (1 - up) * (depth - 1) if depth else (1 - up) * (NX - 1)
        base = pl.multiple_of(plane * PLANE, PLANE)
        tile = sv[plane]

        def emit(j, b, base=base, d=d):
            d[pl.ds(j * NZ, NZ), :] = b * fv[pl.ds(pl.multiple_of(base + j * NZ, NZ), NZ), :]

        spread(tile, emit)
        if depth == 2:
            d[PLANE:, :] = jnp.zeros((SCALES, C), F32)
            d[PLANE:, :NZ] = tile
    for x in range(NX):
        tile = sv[x]
        st = jnp.transpose(tile, (1, 0))
        ends = {
            "gy": [
                jnp.broadcast_to(st[:, y : y + 1], (NZ, C)) * fv[pl.ds(x * PLANE + y * NZ, NZ), :] for y in (0, NY - 1)
            ],
            "gz": [
                jnp.broadcast_to(tile[:, z : z + 1], (NY, C)) * fv[pl.ds(x * PLANE + z, NY, stride=NZ), :]
                for z in (0, NZ - 1)
            ],
        }
        for (axis, kind), send in zip(LOCALS[:-1], sends):
            low, high = ends[axis]
            send[pl.ds(x * LINE[axis], LINE[axis]), :] = jnp.where(side(axis, kind) == 1, high, low)


def aux_kernel(sv, fv, w0, a2, *faces):
    for x in range(NX):

        def emit(j, b, x=x):
            rows = pl.ds(x * PLANE + j * NZ, NZ)
            w0[rows, :] = b * fv[rows, :]
            a2[rows, :] = -2.0 * (b * b)

        spread(sv[x], emit)
    for (axis, kind), face in zip(LOCALS[2:4], faces):
        emit_face(a2, axis, kind, face)


def ghost_aux_kernel(d, a2g):
    def emit(j, b):
        a2g[pl.ds(j * NZ, NZ), :] = -2.0 * (b * b)

    spread(d[PLANE:, :], emit)


def ghost1_kernel(d, a2, weights, a2g, w4, *faces):
    ghost_aux_kernel(d, a2g)
    for (axis, kind), face in zip(LOCALS[:2], faces):
        emit_face(a2, axis, kind, face)
    for layer in range(2):
        w = weights[layer]
        hi = w.astype(jnp.bfloat16)
        lo = (w - hi.astype(F32)).astype(jnp.bfloat16)
        both = jnp.concatenate([hi, lo], axis=1)
        w4[layer, :C, :] = both
        w4[layer, C:, :] = both


def local1_kernel(w0, a2, w1):
    local_pass(True, w0, a2, None, w1)


def local2_kernel(w1, a2, w0, d1, d2, a2g1, w2, p1):
    local_pass(False, w1, a2, w0, w2)
    ghost_pass(True, d1, w0, cross_base(1), d2, a2g1, None, p1)


def local3_kernel(w2, a2, w1, d1, d2, d3, w1g1, a2g1, a2g2, w3, q1, p2):
    local_pass(False, w2, a2, w1, w3)
    ghost_pass(True, d2, d1, 0, d3, a2g2, None, p2)
    ghost_pass(False, w1g1, w1, cross_base(1), p2, a2g1, d1, q1)


def fix1_kernel(w_in, a2, z1, z0, d1, *rest):
    halos, w, sends = rest[:5], rest[5], rest[6:]
    fix_faces(True, w, a2, (z1, z0), halos, d1, sends)
    emit_ghost_lines((d1,), sends)


def fix2_kernel(w_in, a2, z1, z0, d2, p1, a2g1, *rest):
    halos, w, w1g1, sends = rest[:5], rest[5], rest[6], rest[7:]
    fix_lines(True, w1g1, a2g1, halos, 0)
    fix_faces(False, w, a2, (z1, z0), halos, w1g1, sends)
    emit_ghost_lines((w1g1, d2), sends)


def fix3(w, a2, zfaces, q1, a2g1, a2g2, halos, g1, faces):
    copy_plane(q1, 0, g1)
    for (axis, kind), halo in zip(LOCALS[:-1], halos):
        at = plane_line(axis, kind)
        beyond = 0.5 * (a2g2[at, :] * halo[line_rows(axis, 1), :]) + halo[line_rows(axis, 0), :]
        g1[at, :] = g1[at, :] + a2g1[at, :] * beyond
    fix_faces(False, w, a2, zfaces, halos, g1, (*faces, None))


def mixed(layer, ws, a2, thetas, w4, rows, scaled):
    t = None
    for k, w in enumerate(ws):
        term = thetas[layer, k : k + 1, :] * w[rows, :]
        t = term if t is None else t + term
    hi = t.astype(jnp.bfloat16)
    lo = (t - hi.astype(F32)).astype(jnp.bfloat16)
    both = jnp.dot(jnp.concatenate([hi, lo], axis=1), w4[layer], preferred_element_type=F32)
    q = -0.5 * a2[rows, :]
    r = lax.rsqrt(q)
    h = (both[:, :C] + both[:, C:]) * (0.5 * r)
    out = h + h * jnp.tanh(h)
    return (q * r) * out if scaled else out


def mix_planes(layer, ws, a2, thetas, w4, key, dst, scaled, at=0):
    base = side(*key) * ((NX - 1) * PLANE)
    for i in range(PLANE // 256):
        rows = pl.ds(pl.multiple_of(base + i * 256, 256), 256)
        dst[pl.ds(at + i * 256, 256), :] = mixed(layer, ws, a2, thetas, w4, rows, scaled)


def cross_mix_kernel(layer, w3_in, a2, z1, z0, q1, a2g1, a2g2, w0, w1, w2, thetas, w4, *rest):
    halos, w3, d1, faces, g1 = rest[:5], rest[5], rest[6], rest[7:11], rest[11]
    fix3(w3, a2, (z1, z0), q1, a2g1, a2g2, halos, g1, faces)
    mix_planes(layer, (w0, w1, w2, w3), a2, thetas, w4, CROSS, d1, True)


def mix_faces(layer, f, thetas, w4, outs, scaled, planes=(0, NX)):
    for (axis, _), (*ws, a2), out in zip(LOCALS, f, outs):
        start, stop = planes[0] * LINE[axis], planes[1] * LINE[axis]
        size = min(256, stop - start)
        for at in range(start, stop, size):
            rows = pl.ds(at, size)
            out[rows, :] = mixed(layer, ws, a2, thetas, w4, rows, scaled)


def face_mix_kernel(layer, a2, w0, w1, w2, w3, thetas, w4, *rest):
    f, sends = [rest[i :20:4] for i in range(4)], rest[20:]
    mix_faces(layer, f, thetas, w4, sends, True)
    mix_planes(layer, (w0, w1, w2, w3), a2, thetas, w4, LOCALS[-1], sends[-1], True)


def mix_range(layer, scaled, ws, a2, thetas, w4, out, planes, then=None):
    for x in range(*planes):
        for part in range(PLANE // 256):
            rows = pl.ds(x * PLANE + part * 256, 256)
            out[rows, :] = mixed(layer, ws, a2, thetas, w4, rows, scaled)
        if then is not None:
            then(x)


def inner_mix_kernel(layer, scaled, w0, w1, w2, w3, a2, thetas, w4, out):
    mix_range(layer, scaled, (w0, w1, w2, w3), a2, thetas, w4, out, EARLY)


def put_faces(out, faces, planes):
    for (axis, kind), face in zip(LOCALS, faces):
        at = face_slices(axis, kind)
        for g in range(*planes, 4):
            group = range(g, min(g + 4, planes[1]))
            got = [face[at(i)[1], :] for i in group]
            for i, v in zip(group, got):
                out[at(i)[0], :] = v


def merge_kernel(layer, inner, d1, w0, w1, w2, w3, a2, thetas, w4, *rest):
    sends, out, d2, d3 = rest[:5], *rest[5:]
    put_faces(out, sends[:-1], EARLY)
    for key, face in ((CROSS, d1), (LOCALS[-1], sends[-1])):
        base = side(*key) * ((NX - 1) * PLANE)
        for i in range(PLANE // 128):
            out[pl.ds(pl.multiple_of(base + i * 128, 128), 128), :] = face[pl.ds(i * 128, 128), :]
    mix_range(layer, True, (w0, w1, w2, w3), a2, thetas, w4, out, (EARLY[1], NX - 1))
    copy_plane(out, cross_base(2), d2)
    copy_plane(out, cross_base(3), d3)


def last_kernel(layer, w3_in, a2, z1, z0, q1, a2g1, a2g2, w0, w1, w2, thetas, w4, inner, *rest):
    halos, known = rest[:5], rest[5:21]
    (w3, hidden, out), g1, faces, done, sems = rest[21:24], rest[24], rest[25:29], rest[29:33], rest[33]
    fix3(w3, a2, (z1, z0), q1, a2g1, a2g2, halos, g1, faces)

    def copy(i):
        rows = pl.ds(i * PLANE, PLANE)
        return pltpu.make_async_copy(hidden.at[rows, :], out.at[rows, :], sems.at[i])

    f = [(*known[i:12:4], faces[i], known[12 + i]) for i in range(4)]
    mix_faces(layer, f, thetas, w4, done, False, EARLY)
    put_faces(hidden, done, EARLY)
    for i in range(*EARLY):
        copy(i).start()
    ws = (w0, w1, w2, w3)
    for planes in ((0, EARLY[0]), (EARLY[1], NX)):
        mix_range(layer, False, ws, a2, thetas, w4, hidden, planes, lambda x: copy(x).start())
    for i in range(NX):
        copy(i).wait()


def call(kernel, out_shape, args, in_hbm=(), out_hbm=(), scratch=(), aliases=None, mib=1):
    return pl.pallas_call(
        kernel,
        out_shape=out_shape,
        in_specs=[HBM if i in in_hbm else VM for i in range(len(args))],
        out_specs=[HBM if i in out_hbm else VM for i in range(len(out_shape))],
        scratch_shapes=list(scratch),
        input_output_aliases=aliases or {},
        compiler_params=pltpu.CompilerParams(vmem_limit_bytes=mib * MIB),
    )(*args)


def per_device(features, scales, thetas, weights):
    shape = features.shape
    fv, sv = features.reshape(ROWS, C), scales
    feat = pltpu.with_memory_space_constraint(fv, pltpu.HBM)
    block, plane = arr(ROWS), arr(PLANE)
    scales = pltpu.with_memory_space_constraint(scales, pltpu.HBM)
    ghosts = [pltpu.VMEM((PLANE, C), F32)]
    (s1,) = call(
        first_kernel,
        [arr(PLANE + SCALES)],
        (feat, scales),
        in_hbm=(0, 1),
        scratch=[pltpu.VMEM((PLANE, C), F32), pltpu.VMEM((NY, NZ), F32), pltpu.SemaphoreType.DMA((2,))],
    )
    s2, s3, *sends = call(start_kernel, [arr(PLANE + SCALES), plane] + locals_out(0), (fv, sv))
    for layer in range(2):
        last = layer == 1
        if last:
            w0, s2, s3 = call(
                functools.partial(merge_kernel, 0),
                [block, plane, plane],
                (inner, s1, w0, w1, w2, w3, a2, thetas, w4, *sends),
                aliases={0: 0},
            )
        known = [sends[:4]]
        (d1,), halos, (d2,) = exchange(sends, cross=s1, late=s2)
        if not last:
            w0, a2, *az = call(aux_kernel, [block, block] + locals_out(0)[2:4], (sv, fv))
            main = (a2, *az)
        (w1,) = call(local1_kernel, [block], (w0, a2))
        w1, *sends = call(fix1_kernel, [block] + locals_out(1), (w1, *main, d1, *halos), aliases={0: 0})
        known.append(sends[:4])
        _, halos, (d3,) = exchange(sends, late=s3)
        if not last:
            w4 = jax.ShapeDtypeStruct((2, 2 * C, 2 * C), jnp.bfloat16)
            a2g1, w4, *ay = call(ghost1_kernel, [plane, w4] + locals_out(0)[:2], (d1, a2, weights))
            af = (*ay, *az)
        w2, p1 = call(local2_kernel, [block, plane], (w1, a2, w0, d1, d2, a2g1))
        w2, w1g1, *sends = call(
            fix2_kernel, [block, plane] + locals_out(2), (w2, *main, d2, p1, a2g1, *halos), aliases={0: 0, 5: 1}
        )
        known.append(sends[:4])
        _, halos, _ = exchange(sends)
        if not last:
            (a2g2,) = call(ghost_aux_kernel, [plane], (d2,))
        w3, q1 = call(local3_kernel, [block, plane], (w2, a2, w1, d1, d2, d3, w1g1, a2g1, a2g2), scratch=ghosts)
        (inner,) = call(functools.partial(inner_mix_kernel, layer, not last), [block], (w0, w1, w2, w3, a2, thetas, w4))
        tail = (w3, *main, q1, a2g1, a2g2, w0, w1, w2, thetas, w4)
        if not last:
            w3, s1, *faces = call(
                functools.partial(cross_mix_kernel, layer),
                [block, plane] + locals_out(0)[:4],
                (*tail, *halos),
                scratch=ghosts,
                aliases={0: 0},
            )
            sends = call(
                functools.partial(face_mix_kernel, layer),
                locals_out(0),
                (a2, w0, w1, w2, w3, thetas, w4, *sum(map(list, known), []), *faces, *af),
            )
        else:
            small = [pltpu.VMEM(a.shape, F32) for a in locals_out(0)[:4]]
            n = len(tail)
            _, _, out = call(
                functools.partial(last_kernel, layer),
                [block, block, block],
                (*tail, inner, *halos, *sum(map(list, known), []), *af),
                out_hbm=(2,),
                scratch=ghosts + small + small + [pltpu.SemaphoreType.DMA((NX,))],
                mib=3,
                aliases={0: 0, n: 1},
            )
    return out.reshape(shape)


def solution(mesh):
    return jax.shard_map(
        per_device,
        mesh=mesh,
        in_specs=(P(*AXES, None), P(*AXES), P(), P()),
        out_specs=P(*AXES, None),
        check_vma=False,
    )
```

```python
import functools

import jax
import jax.numpy as jnp
from jax import lax
from jax.experimental import pallas as pl
from jax.experimental.pallas import tpu as pltpu
from jax.sharding import PartitionSpec as P


AXES = ("gx", "gy", "gz")
NX, NY, NZ, C = 16, 16, 32, 128
PLANE = NY * NZ
ROWS = NX * PLANE
FACE = {"gx": PLANE, "gy": NX * NZ, "gz": NX * NY}
LINE = {"gy": NZ, "gz": NY}
CROSS = ("gx", 1)
LOCALS = (("gy", 0), ("gy", 1), ("gz", 1), ("gz", 0), ("gx", 0))
EARLY = ((1, 7), (1, 9))
SCALES = 16

F32 = jnp.float32
VM = pl.BlockSpec(memory_space=pltpu.VMEM)
HBM = pl.BlockSpec(memory_space=pltpu.HBM)
MIB = 1024 * 1024


def arr(rows, cols=C, dtype=F32):
    return jax.ShapeDtypeStruct((rows, cols), dtype)


def locals_out(lines):
    return [arr(FACE[a] + lines * LINE.get(a, 0)) for a, _ in LOCALS]


def swap(x, axis, kind):
    n = lax.axis_size(axis)
    pairs = []
    for i in range(kind, n + kind, 2):
        a, b = i % n, (i + 1) % n
        pairs += [(a, b), (b, a)]
    return lax.ppermute(x, axis, pairs)


def exchange(sends, cross=None, late=None):
    first = [] if cross is None else [swap(cross, *CROSS)]
    got = [swap(s, a, k) for s, (a, k) in zip(sends, LOCALS)]
    last = [] if late is None else [swap(late, *CROSS)]
    return first, got, last


def side(axis, kind):
    odd = lax.rem(lax.axis_index(axis), 2)
    return odd if kind else 1 - odd


def face_slices(axis, kind):
    up = side(axis, kind)
    if axis == "gx":
        base = up * ((NX - 1) * PLANE)
        return lambda i: (pl.ds(pl.multiple_of(base + i * NZ, NZ), NZ), pl.ds(pl.multiple_of(i * NZ, NZ), NZ))
    if axis == "gy":
        base = up * ((NY - 1) * NZ)
        return lambda i: (pl.ds(pl.multiple_of(base + i * PLANE, NZ), NZ), pl.ds(pl.multiple_of(i * NZ, NZ), NZ))
    base = up * (NZ - 1)
    return lambda i: (pl.ds(base + i * PLANE, NY, stride=NZ), pl.ds(pl.multiple_of(i * NY, NY), NY))


def plane_line(axis, kind):
    up = side(axis, kind)
    if axis == "gy":
        return pl.ds(pl.multiple_of(up * ((NY - 1) * NZ), NZ), NZ)
    return pl.ds(up * (NZ - 1), NY, stride=NZ)


def line_rows(axis, i):
    return pl.ds(FACE[axis] + i * LINE[axis], LINE[axis])


def cross_base(depth):
    up = side(*CROSS)
    return pl.multiple_of(up * ((NX - depth) * PLANE) + (1 - up) * ((depth - 1) * PLANE), PLANE)


def copy_plane(src, base, dst):
    for i in range(PLANE // 128):
        rows = pl.ds(i * 128, 128)
        dst[rows, :] = src[pl.ds(pl.multiple_of(base + i * 128, 128), 128), :]


def batches(axis):
    size = 8 if axis == "gz" else 4
    return [range(g, g + size) for g in range(0, NX, size)]


def emit_face(w, axis, kind, send):
    at = face_slices(axis, kind)
    for group in batches(axis):
        got = [w[at(i)[0], :] for i in group]
        for i, v in zip(group, got):
            send[at(i)[1], :] = v


def fix_faces(half, w, a2, zfaces, halos, cross, sends):
    local = list(zip(LOCALS, halos, sends))
    plain = [(CROSS, cross)] + [(k, h) for k, h, _ in local if k[0] == "gx"] + [(k, h) for k, h, _ in local if k[0] == "gy"]
    for key, halo in plain:
        at = face_slices(*key)
        for group in batches(key[0]):
            got = []
            for i in group:
                dst, src = at(i)
                r = a2[dst, :] * halo[src, :]
                got.append(w[dst, :] + (0.5 * r if half else r))
            for i, v in zip(group, got):
                w[at(i)[0], :] = v
    for ((key, halo, send), face) in zip([t for t in local if t[0][0] == "gz"], zfaces):
        at = face_slices(*key)
        for group in batches("gz"):
            got = []
            for i in group:
                dst, src = at(i)
                r = face[src, :] * halo[src, :]
                got.append(w[dst, :] + (0.5 * r if half else r))
            for i, v in zip(group, got):
                w[at(i)[0], :] = v
                send[at(i)[1], :] = v
    for (axis, kind), _, send in local:
        if axis != "gz" and send is not None:
            emit_face(w, axis, kind, send)


def emit_ghost_lines(ghosts, sends):
    for (axis, kind), send in zip(LOCALS, sends):
        if axis != "gx":
            for i, g in enumerate(ghosts):
                send[line_rows(axis, i), :] = g[plane_line(axis, kind), :]


def fix_lines(half, g, a2, halos, i):
    for (axis, kind), halo in zip(LOCALS, halos):
        if axis == "gx":
            continue
        at = plane_line(axis, kind)
        r = a2[at, :] * halo[line_rows(axis, i), :]
        g[at, :] = g[at, :] + (0.5 * r if half else r)


def yz_sums(w, base, emit):
    sub = lax.broadcasted_iota(jnp.int32, (8, C), 0)
    top, bottom = sub == 0, sub == 7
    nv = NZ // 8

    def at(y):
        return [w[pl.ds(pl.multiple_of(base + y * NZ + 8 * k, 8), 8), :] for k in range(nv)]

    below, here = None, at(0)
    for y in range(NY):
        above = at(y + 1) if y + 1 < NY else None
        dn = [pltpu.roll(v, 1, 0) for v in here]
        up = [pltpu.roll(v, 7, 0) for v in here]
        for k in range(nv):
            n = jnp.where(top, dn[k - 1] if k else 0.0, dn[k]) + jnp.where(
                bottom, up[k + 1] if k + 1 < nv else 0.0, up[k]
            )
            for other in (below, above):
                if other is not None:
                    n = n + other[k]
            emit(y * NZ + 8 * k, n)
        below, here = here, above


def rows8(base, r):
    return pl.ds(pl.multiple_of(base + r, 8), 8)


def local_pass(half, w, a2, prior, out):
    def plane(base, lo, hi):
        def emit(r, n):
            if lo:
                n = n + w[rows8(base, r - PLANE), :]
            if hi:
                n = n + w[rows8(base, r + PLANE), :]
            v = a2[rows8(base, r), :] * n
            out[rows8(base, r), :] = 0.5 * v if half else v - prior[rows8(base, r), :]

        yz_sums(w, base, emit)

    plane(0, False, True)
    lax.fori_loop(1, NX - 1, lambda i, c: (plane(pl.multiple_of(i * PLANE, PLANE), True, True), c)[1], 0)
    plane((NX - 1) * PLANE, True, False)


def ghost_pass(half, g, inner, inner_base, outer, a2, prior, out):
    def emit(r, n):
        v = a2[rows8(0, r), :] * (n + inner[rows8(inner_base, r), :] + outer[rows8(0, r), :])
        out[rows8(0, r), :] = 0.5 * v if half else v - prior[rows8(0, r), :]

    yz_sums(g, 0, emit)


def spread(tile, emit):
    st = jnp.transpose(tile, (1, 0))
    for j in range(NY):
        emit(j, jnp.broadcast_to(st[:NZ, j : j + 1], (NZ, C)))


def first_kernel(feat, scales, d1, buf, sv, sems):
    up = side(*CROSS)
    two = [
        pltpu.make_async_copy(scales.at[up * (NX - 1)], sv, sems.at[0]),
        pltpu.make_async_copy(feat.at[pl.ds(cross_base(1), PLANE), :], buf, sems.at[1]),
    ]
    for c in two:
        c.start()
    two[0].wait()
    tile = sv[...]
    d1[PLANE:, :] = jnp.zeros((SCALES, C), F32)
    d1[PLANE:, :NZ] = tile
    two[1].wait()

    def emit(j, b):
        rows = pl.ds(j * NZ, NZ)
        d1[rows, :] = b * buf[rows, :]

    spread(tile, emit)


def start_kernel(fv, sv, d2, d3, *sends):
    up = side(*CROSS)
    for depth, d in ((2, d2), (3, d3), (0, sends[-1])):
        plane = up * (NX - depth) + (1 - up) * (depth - 1) if depth else (1 - up) * (NX - 1)
        base = pl.multiple_of(plane * PLANE, PLANE)
        tile = sv[plane]

        def emit(j, b, base=base, d=d):
            d[pl.ds(j * NZ, NZ), :] = b * fv[pl.ds(pl.multiple_of(base + j * NZ, NZ), NZ), :]

        spread(tile, emit)
        if depth == 2:
            d[PLANE:, :] = jnp.zeros((SCALES, C), F32)
            d[PLANE:, :NZ] = tile
    for x in range(NX):
        tile = sv[x]
        st = jnp.transpose(tile, (1, 0))
        ends = {
            "gy": [
                jnp.broadcast_to(st[:, y : y + 1], (NZ, C)) * fv[pl.ds(x * PLANE + y * NZ, NZ), :] for y in (0, NY - 1)
            ],
            "gz": [
                jnp.broadcast_to(tile[:, z : z + 1], (NY, C)) * fv[pl.ds(x * PLANE + z, NY, stride=NZ), :]
                for z in (0, NZ - 1)
            ],
        }
        for (axis, kind), send in zip(LOCALS[:-1], sends):
            low, high = ends[axis]
            send[pl.ds(x * LINE[axis], LINE[axis]), :] = jnp.where(side(axis, kind) == 1, high, low)


def aux_kernel(sv, fv, w0, a2, *faces):
    for x in range(NX):

        def emit(j, b, x=x):
            rows = pl.ds(x * PLANE + j * NZ, NZ)
            w0[rows, :] = b * fv[rows, :]
            a2[rows, :] = -2.0 * (b * b)

        spread(sv[x], emit)
    for (axis, kind), face in zip(LOCALS[2:4], faces):
        emit_face(a2, axis, kind, face)


def ghost_aux_kernel(d, a2g):
    def emit(j, b):
        a2g[pl.ds(j * NZ, NZ), :] = -2.0 * (b * b)

    spread(d[PLANE:, :], emit)


def ghost1_kernel(d, a2, weights, a2g, w4, *faces):
    ghost_aux_kernel(d, a2g)
    for (axis, kind), face in zip(LOCALS[:2], faces):
        emit_face(a2, axis, kind, face)
    for layer in range(2):
        w = weights[layer]
        hi = w.astype(jnp.bfloat16)
        lo = (w - hi.astype(F32)).astype(jnp.bfloat16)
        both = jnp.concatenate([hi, lo], axis=1)
        w4[layer, :C, :] = both
        w4[layer, C:, :] = both


def local1_kernel(w0, a2, w1):
    local_pass(True, w0, a2, None, w1)


def local2_kernel(w1, a2, w0, d1, d2, a2g1, w2, p1):
    local_pass(False, w1, a2, w0, w2)
    ghost_pass(True, d1, w0, cross_base(1), d2, a2g1, None, p1)


def local3_kernel(w2, a2, w1, d1, d2, d3, w1g1, a2g1, a2g2, w3, q1, p2):
    local_pass(False, w2, a2, w1, w3)
    ghost_pass(True, d2, d1, 0, d3, a2g2, None, p2)
    ghost_pass(False, w1g1, w1, cross_base(1), p2, a2g1, d1, q1)


def fix1_kernel(w_in, a2, z1, z0, d1, *rest):
    halos, w, sends = rest[:5], rest[5], rest[6:]
    fix_faces(True, w, a2, (z1, z0), halos, d1, sends)
    emit_ghost_lines((d1,), sends)


def fix2_kernel(w_in, a2, z1, z0, d2, p1, a2g1, *rest):
    halos, w, w1g1, sends = rest[:5], rest[5], rest[6], rest[7:]
    fix_lines(True, w1g1, a2g1, halos, 0)
    fix_faces(False, w, a2, (z1, z0), halos, w1g1, sends)
    emit_ghost_lines((w1g1, d2), sends)


def fix3(w, a2, zfaces, q1, a2g1, a2g2, halos, g1, faces):
    copy_plane(q1, 0, g1)
    for (axis, kind), halo in zip(LOCALS[:-1], halos):
        at = plane_line(axis, kind)
        beyond = 0.5 * (a2g2[at, :] * halo[line_rows(axis, 1), :]) + halo[line_rows(axis, 0), :]
        g1[at, :] = g1[at, :] + a2g1[at, :] * beyond
    fix_faces(False, w, a2, zfaces, halos, g1, (*faces, None))


def mixed(layer, ws, a2, thetas, w4, rows, scaled):
    t = None
    for k, w in enumerate(ws):
        term = thetas[layer, k : k + 1, :] * w[rows, :]
        t = term if t is None else t + term
    hi = t.astype(jnp.bfloat16)
    lo = (t - hi.astype(F32)).astype(jnp.bfloat16)
    both = jnp.dot(jnp.concatenate([hi, lo], axis=1), w4[layer], preferred_element_type=F32)
    q = -0.5 * a2[rows, :]
    r = lax.rsqrt(q)
    h = (both[:, :C] + both[:, C:]) * (0.5 * r)
    out = h + h * jnp.tanh(h)
    return (q * r) * out if scaled else out


def mix_planes(layer, ws, a2, thetas, w4, key, dst, scaled, at=0):
    base = side(*key) * ((NX - 1) * PLANE)
    for i in range(PLANE // 256):
        rows = pl.ds(pl.multiple_of(base + i * 256, 256), 256)
        dst[pl.ds(at + i * 256, 256), :] = mixed(layer, ws, a2, thetas, w4, rows, scaled)


def cross_mix_kernel(layer, w3_in, a2, z1, z0, q1, a2g1, a2g2, w0, w1, w2, thetas, w4, *rest):
    halos, w3, d1, faces, g1 = rest[:5], rest[5], rest[6], rest[7:11], rest[11]
    fix3(w3, a2, (z1, z0), q1, a2g1, a2g2, halos, g1, faces)
    mix_planes(layer, (w0, w1, w2, w3), a2, thetas, w4, CROSS, d1, True)


def mix_faces(layer, f, thetas, w4, outs, scaled, planes=(0, NX)):
    for (axis, _), (*ws, a2), out in zip(LOCALS, f, outs):
        start, stop = planes[0] * LINE[axis], planes[1] * LINE[axis]
        size = min(256, stop - start)
        for at in range(start, stop, size):
            rows = pl.ds(at, size)
            out[rows, :] = mixed(layer, ws, a2, thetas, w4, rows, scaled)


def face_mix_kernel(layer, a2, w0, w1, w2, w3, thetas, w4, *rest):
    f, sends = [rest[i :20:4] for i in range(4)], rest[20:]
    mix_faces(layer, f, thetas, w4, sends, True)
    mix_planes(layer, (w0, w1, w2, w3), a2, thetas, w4, LOCALS[-1], sends[-1], True)


def mix_range(layer, scaled, ws, a2, thetas, w4, out, planes, then=None):
    for x in range(*planes):
        for part in range(PLANE // 256):
            rows = pl.ds(x * PLANE + part * 256, 256)
            out[rows, :] = mixed(layer, ws, a2, thetas, w4, rows, scaled)
        if then is not None:
            then(x)


def inner_mix_kernel(layer, scaled, w0, w1, w2, w3, a2, thetas, w4, out):
    mix_range(layer, scaled, (w0, w1, w2, w3), a2, thetas, w4, out, EARLY[layer])


def put_faces(out, faces, planes):
    for (axis, kind), face in zip(LOCALS, faces):
        at = face_slices(axis, kind)
        for g in range(*planes, 4):
            group = range(g, min(g + 4, planes[1]))
            got = [face[at(i)[1], :] for i in group]
            for i, v in zip(group, got):
                out[at(i)[0], :] = v


def merge_kernel(layer, inner, d1, w0, w1, w2, w3, a2, thetas, w4, *rest):
    sends, out, d2, d3 = rest[:5], *rest[5:]
    put_faces(out, sends[:-1], EARLY[layer])
    for key, face in ((CROSS, d1), (LOCALS[-1], sends[-1])):
        base = side(*key) * ((NX - 1) * PLANE)
        for i in range(PLANE // 128):
            out[pl.ds(pl.multiple_of(base + i * 128, 128), 128), :] = face[pl.ds(i * 128, 128), :]
    mix_range(layer, True, (w0, w1, w2, w3), a2, thetas, w4, out, (EARLY[layer][1], NX - 1))
    copy_plane(out, cross_base(2), d2)
    copy_plane(out, cross_base(3), d3)


def last_kernel(layer, w3_in, a2, z1, z0, q1, a2g1, a2g2, w0, w1, w2, thetas, w4, inner, *rest):
    halos, known = rest[:5], rest[5:21]
    (w3, hidden, out), g1, faces, done, sems = rest[21:24], rest[24], rest[25:29], rest[29:33], rest[33]
    fix3(w3, a2, (z1, z0), q1, a2g1, a2g2, halos, g1, faces)

    def copy(i):
        rows = pl.ds(i * PLANE, PLANE)
        return pltpu.make_async_copy(hidden.at[rows, :], out.at[rows, :], sems.at[i])

    f = [(*known[i:12:4], faces[i], known[12 + i]) for i in range(4)]
    early = EARLY[layer]
    mix_faces(layer, f, thetas, w4, done, False, early)
    put_faces(hidden, done, early)
    for i in range(*early):
        copy(i).start()
    ws = (w0, w1, w2, w3)
    for planes in ((0, early[0]), (early[1], NX)):
        mix_range(layer, False, ws, a2, thetas, w4, hidden, planes, lambda x: copy(x).start())
    for i in range(NX):
        copy(i).wait()


def call(kernel, out_shape, args, in_hbm=(), out_hbm=(), scratch=(), aliases=None, mib=1):
    return pl.pallas_call(
        kernel,
        out_shape=out_shape,
        in_specs=[HBM if i in in_hbm else VM for i in range(len(args))],
        out_specs=[HBM if i in out_hbm else VM for i in range(len(out_shape))],
        scratch_shapes=list(scratch),
        input_output_aliases=aliases or {},
        compiler_params=pltpu.CompilerParams(vmem_limit_bytes=mib * MIB),
    )(*args)


def per_device(features, scales, thetas, weights):
    shape = features.shape
    fv, sv = features.reshape(ROWS, C), scales
    feat = pltpu.with_memory_space_constraint(fv, pltpu.HBM)
    block, plane = arr(ROWS), arr(PLANE)
    scales = pltpu.with_memory_space_constraint(scales, pltpu.HBM)
    ghosts = [pltpu.VMEM((PLANE, C), F32)]
    (s1,) = call(
        first_kernel,
        [arr(PLANE + SCALES)],
        (feat, scales),
        in_hbm=(0, 1),
        scratch=[pltpu.VMEM((PLANE, C), F32), pltpu.VMEM((NY, NZ), F32), pltpu.SemaphoreType.DMA((2,))],
    )
    s2, s3, *sends = call(start_kernel, [arr(PLANE + SCALES), plane] + locals_out(0), (fv, sv))
    for layer in range(2):
        last = layer == 1
        if last:
            w0, s2, s3 = call(
                functools.partial(merge_kernel, 0),
                [block, plane, plane],
                (inner, s1, w0, w1, w2, w3, a2, thetas, w4, *sends),
                aliases={0: 0},
            )
        known = [sends[:4]]
        (d1,), halos, (d2,) = exchange(sends, cross=s1, late=s2)
        if not last:
            w0, a2, *az = call(aux_kernel, [block, block] + locals_out(0)[2:4], (sv, fv))
            main = (a2, *az)
        (w1,) = call(local1_kernel, [block], (w0, a2))
        w1, *sends = call(fix1_kernel, [block] + locals_out(1), (w1, *main, d1, *halos), aliases={0: 0})
        known.append(sends[:4])
        _, halos, (d3,) = exchange(sends, late=s3)
        if not last:
            w4 = jax.ShapeDtypeStruct((2, 2 * C, 2 * C), jnp.bfloat16)
            a2g1, w4, *ay = call(ghost1_kernel, [plane, w4] + locals_out(0)[:2], (d1, a2, weights))
            af = (*ay, *az)
        w2, p1 = call(local2_kernel, [block, plane], (w1, a2, w0, d1, d2, a2g1))
        w2, w1g1, *sends = call(
            fix2_kernel, [block, plane] + locals_out(2), (w2, *main, d2, p1, a2g1, *halos), aliases={0: 0, 5: 1}
        )
        known.append(sends[:4])
        _, halos, _ = exchange(sends)
        if not last:
            (a2g2,) = call(ghost_aux_kernel, [plane], (d2,))
        w3, q1 = call(local3_kernel, [block, plane], (w2, a2, w1, d1, d2, d3, w1g1, a2g1, a2g2), scratch=ghosts)
        (inner,) = call(functools.partial(inner_mix_kernel, layer, not last), [block], (w0, w1, w2, w3, a2, thetas, w4))
        tail = (w3, *main, q1, a2g1, a2g2, w0, w1, w2, thetas, w4)
        if not last:
            w3, s1, *faces = call(
                functools.partial(cross_mix_kernel, layer),
                [block, plane] + locals_out(0)[:4],
                (*tail, *halos),
                scratch=ghosts,
                aliases={0: 0},
            )
            sends = call(
                functools.partial(face_mix_kernel, layer),
                locals_out(0),
                (a2, w0, w1, w2, w3, thetas, w4, *sum(map(list, known), []), *faces, *af),
            )
        else:
            small = [pltpu.VMEM(a.shape, F32) for a in locals_out(0)[:4]]
            n = len(tail)
            _, _, out = call(
                functools.partial(last_kernel, layer),
                [block, block, block],
                (*tail, inner, *halos, *sum(map(list, known), []), *af),
                out_hbm=(2,),
                scratch=ghosts + small + small + [pltpu.SemaphoreType.DMA((NX,))],
                mib=3,
                aliases={0: 0, n: 1},
            )
    return out.reshape(shape)


def solution(mesh):
    return jax.shard_map(
        per_device,
        mesh=mesh,
        in_specs=(P(*AXES, None), P(*AXES), P(), P()),
        out_specs=P(*AXES, None),
        check_vma=False,
    )
```
